32 devices in a mesh: tm: 8 (over z, y), space: 4 (over x, core).
Axes of the slice: x: 2, y: 2, z: 4, core: 2. Of those that a mesh axis runs over, the one named last changes fastest.
Arguments:
- residual: float32 [8, 2, 1024, 1024], P('tm', None, 'space'), may hold values from -0.875 to 0.875
- counts: int32 [8], P('tm'), may hold values from 1 to 4
Outputs:
- fields: float32 [8, 2, 1024, 1024], P('tm', None, 'space')
The draws below stay inside these ranges and needn't reach their ends.
All inputs are finite; a program needn't handle non-finite values.
Results may differ from the reference program's by a relative error of at most 0.0003.
Values sent between devices are 32-bit elements; how exact they have to be, the bound alone decides.
No kernel may reach another device: no remote copies, remote signals or barrier semaphores. Data moves between devices by JAX's collectives and lax.ppermute only.
A program may use at most 320 MiB of HBM per device.

```python
import jax
import jax.numpy as jnp
from jax import lax

NX = 1024
NY = 1024
NT = 8


def set_ends(array, stream_key, least, high):
    longest = array.shape.index(max(array.shape))
    spots = []
    for shift in (0, 1):
        where = [jax.random.randint(jax.random.fold_in(stream_key, axis), (), 0, length) for axis, length in enumerate(array.shape)]
        where[longest] = (where[longest] + shift) % array.shape[longest]
        spots.append(tuple(where))
    return array.at[spots[0]].set(least).at[spots[1]].set(high)


def block_scale(rng, shape, shards, low, high):
    level, own = 1.0, jax.random.fold_in(rng, 6)
    for position, shards_of in shards:
        draws = jnp.exp(jax.random.uniform(jax.random.fold_in(own, position), (shards_of,), jnp.float32, low / len(shards), high / len(shards)))
        level = level * jnp.repeat(draws, shape[position] // shards_of).reshape([-1 if axis == position else 1 for axis in range(len(shape))])
    return level


def scatter_about(stream_key, shape, width, limit, shards=(), kind=jnp.bfloat16):
    gain = block_scale(stream_key, shape, shards, -0.22, 0.18) if shards else 1.0
    drawn = jax.random.normal(stream_key, shape, jnp.float32) * width * gain
    return jnp.minimum(jnp.maximum(drawn, -limit), limit).astype(kind)


def setup_inputs(seed: int = 0) -> dict:
    streams_of = jax.random.split(jax.random.key(seed), 3)
    return {
        "residual": scatter_about(streams_of[0], (NT, 2, NX, NY), 0.15, 0.875, ((0, 8), (2, 4)), jnp.float32),
        "counts": set_ends(jax.random.randint(streams_of[1], (NT,), 1, 5), jax.random.fold_in(streams_of[1], 1), 1, 4).astype(jnp.int32),
    }


phase_rate = 0.004

def signed_wave(indices, length):
    return jnp.where(indices < length // 2, indices, indices - length).astype(jnp.float32)

def reference(residual, counts):
    wave_x = signed_wave(jnp.arange(NX, dtype=jnp.int32), NX)
    wave_y = signed_wave(jnp.arange(NY, dtype=jnp.int32), NY)
    modulus = jnp.sqrt(wave_x[:, None] * wave_x[:, None] + wave_y[None, :] * wave_y[None, :])

    def advance(carried, inputs):
        source, step_count = inputs
        phases = phase_rate * step_count.astype(jnp.float32) * modulus
        cosine = jnp.cos(phases)
        sine_part = jnp.sin(phases)
        spectrum = jnp.fft.fft2(source, axes=(1, 2))
        first_part = cosine * carried[0] + sine_part * carried[1] + spectrum[0]
        second_part = cosine * carried[1] - sine_part * carried[0] + spectrum[1]
        updated = jnp.stack([first_part, second_part])
        physical = jnp.real(jnp.fft.ifft2(updated, axes=(1, 2))).astype(residual.dtype)
        return (updated, physical)
    initial = jnp.zeros_like(jnp.fft.fft2(residual[0], axes=(1, 2)))
    last_state, fields = lax.scan(advance, initial, (residual, counts))
    return fields
```

```python
import functools
import math

import jax
import jax.numpy as jnp
import numpy as np
from jax import lax
from jax.experimental import pallas as pl
from jax.experimental.pallas import tpu as pltpu
from jax.sharding import Mesh
from jax.sharding import PartitionSpec as P

phase_rate = 0.004
f32 = jnp.float32
bf16 = jnp.bfloat16
NN = (((1,), (0,)), ((), ()))
NT = (((1,), (1,)), ((), ()))
TN = (((0,), (0,)), ((), ()))
SIN = (3.14159274, -5.1677103, 2.55007744, -0.598291218, 0.0776574388)
COS = (1.0, -4.93480206, 4.05870914, -1.335212, 0.23493728, -0.0243962663)


def cas_tables(length):
    quarter = length // 4
    m = np.arange(quarter, dtype=np.int64)
    j = np.arange(quarter, dtype=np.int64)

    def cas(k, sign=1):
        angle = sign * 2.0 * np.pi * ((k[:, None] * j[None, :]) % length) / length
        return np.cos(angle) + np.sin(angle)

    odd = np.block(
        [
            [cas(4 * m + 1), cas(4 * m + 1, -1)],
            [cas(4 * m + 3), -cas(4 * m + 3, -1)],
        ]
    )
    tables = []
    for table in (cas(4 * m), cas(4 * m + 2), odd):
        table = table.astype(np.float32)
        high = table.astype(jnp.bfloat16)
        low = (table - high.astype(np.float32)).astype(jnp.bfloat16)
        tables += [high, low]
    return tables


def halves(value):
    high = value.astype(bf16)
    return high, (value - high.astype(f32)).astype(bf16)


def product(left, right, form):
    dot = functools.partial(lax.dot_general, dimension_numbers=form, preferred_element_type=f32)
    return dot(left[0], right[0]) + dot(left[0], right[1]) + dot(left[1], right[0])


def fold(parts):
    even, cross = parts[0] + parts[2], parts[1] + parts[3]
    return even + cross, even - cross


def fold_odd(parts):
    return jnp.concatenate([parts[0] - parts[2], parts[1] - parts[3]], axis=-1)


def signed_wave(indices, length):
    return jnp.where(indices < length // 2, indices, indices - length).astype(f32)


def wave_at(spot, length):
    quarter = length // 4
    block = spot // quarter
    return 4 * (spot % quarter) + jnp.where(block == 1, 2, jnp.where(block == 2, 1, block))


def modulus_at(start, shape, length_x, length_y):
    place_y = start + lax.broadcasted_iota(jnp.int32, shape, 0)
    place_x = lax.broadcasted_iota(jnp.int32, shape, 1)
    wave_y = signed_wave(wave_at(place_y, length_y), length_y)
    wave_x = signed_wave(wave_at(place_x, length_x), length_x)
    return jnp.sqrt(wave_x * wave_x + wave_y * wave_y)


def turn(angle):
    part = angle - jnp.round(angle)
    square = part * part
    sine = jnp.full_like(square, SIN[-1])
    for factor in SIN[-2::-1]:
        sine = sine * square + factor
    sine = sine * part
    cosine = jnp.full_like(square, COS[-1])
    for factor in COS[-2::-1]:
        cosine = cosine * square + factor
    return 1.0 - 2.0 * sine * sine, 2.0 * sine * cosine


def place(odd, rows, length_y):
    point = lax.axis_index("point")
    band = point * lax.axis_size("space") + lax.axis_index("space")
    return odd * (length_y // 2) + band * rows, point


def rate_of(n, point, count_refs):
    points = len(count_refs)
    shift = lax.rem(point + points - n, points)
    count = count_refs[0][0]
    for d in range(1, points):
        count = jnp.where(shift == d, count_refs[d][0], count)
    return count.astype(f32) * (phase_rate / (2.0 * math.pi))


def forward_y(odd, x_ref, *refs):
    tables, out = [ref[...] for ref in refs[:-1]], refs[-1]
    quarter = x_ref.shape[-1] // 4
    bands, _, rows, slab = out.shape
    for part in range(2):
        pieces = [x_ref[part, :, q * quarter : (q + 1) * quarter] for q in range(4)]
        if odd:
            result = product(tables, halves(fold_odd(pieces)), NT)
            out[:, part] = result.reshape(bands, rows, slab)
        else:
            total, alternate = fold(pieces)
            half = bands // 2
            out[:half, part] = product(tables[:2], halves(total), NT).reshape(half, rows, slab)
            out[half:, part] = product(tables[2:], halves(alternate), NT).reshape(half, rows, slab)


def forward_x(odd, length_y, points, *refs):
    count_refs, (r_ref, *refs) = refs[:points], refs[points:]
    tables, (spectra, last) = [ref[...] for ref in refs[:-2]], refs[-2:]
    points, spaces, _, rows, slab = r_ref.shape
    start, point = place(odd, rows, length_y)
    rates = [rate_of(n, point, count_refs) for n in range(points)]
    length_x = spaces * slab
    quarter = length_x // 4
    count = points * 2 * rows
    if spaces == 4:
        pieces = [r_ref[:, s].reshape(count, slab) for s in range(4)]
    else:
        whole = jnp.concatenate([r_ref[:, s].reshape(count, slab) for s in range(spaces)], axis=-1)
        pieces = [whole[:, q * quarter : (q + 1) * quarter] for q in range(4)]
    total, alternate = fold(pieces)
    shape = (points, 2, rows, quarter)
    spectra[..., :quarter] = product(halves(total), tables[:2], NT).reshape(shape)
    spectra[..., quarter : 2 * quarter] = product(halves(alternate), tables[2:4], NT).reshape(shape)
    mixed = product(halves(fold_odd(pieces)), tables[4:], NT)
    spectra[..., 2 * quarter :] = mixed.reshape(points, 2, rows, 2 * quarter)
    block = math.gcd(rows, 8)

    def step(index, _):
        here = pl.ds(pl.multiple_of(index * block, block), block)
        modulus = modulus_at(start + index * block, (block, length_x), length_x, length_y)
        first, second = spectra[0, 0, here, :], spectra[0, 1, here, :]
        for n in range(1, points):
            cosine, sine = turn(rates[n] * modulus)
            first, second = (
                cosine * first + sine * second + spectra[n, 0, here, :],
                cosine * second - sine * first + spectra[n, 1, here, :],
            )
        last[0, here, :] = first
        last[1, here, :] = second
        return 0

    lax.fori_loop(0, rows // block, step, 0)


def finish_x(odd, length_y, points, *refs):
    count_refs, (spectra, carry, *refs) = refs[:points], refs[points:]
    tables, (out, states) = [ref[...] for ref in refs[:-2]], refs[-2:]
    points, spaces, _, rows, slab = out.shape
    length_x = spaces * slab
    quarter = length_x // 4
    count = points * 2 * rows
    block = math.gcd(rows, 8)
    scaling = 1.0 / (length_x * length_y)
    start, point = place(odd, rows, length_y)
    rates = [rate_of(n, point, count_refs) for n in range(points)]

    def step(index, _):
        here = pl.ds(pl.multiple_of(index * block, block), block)
        modulus = modulus_at(start + index * block, (block, length_x), length_x, length_y)
        first, second = carry[0, here, :], carry[1, here, :]
        for n in range(points):
            cosine, sine = turn(rates[n] * modulus)
            first, second = (
                cosine * first + sine * second + spectra[n, 0, here, :],
                cosine * second - sine * first + spectra[n, 1, here, :],
            )
            states[n, 0, here, :] = first * scaling
            states[n, 1, here, :] = second * scaling
        return 0

    lax.fori_loop(0, rows // block, step, 0)
    total = product(halves(states[..., :quarter].reshape(count, quarter)), tables[:2], NN)
    alternate = product(halves(states[..., quarter : 2 * quarter].reshape(count, quarter)), tables[2:4], NN)
    mixed = product(halves(states[..., 2 * quarter :].reshape(count, 2 * quarter)), tables[4:], NN)
    plus, minus = total + alternate, total - alternate
    straight, crossed = mixed[:, :quarter], mixed[:, quarter:]
    results = [plus + straight, minus + crossed, plus - straight, minus - crossed]
    if spaces != 4:
        whole = jnp.concatenate(results, axis=-1)
        results = [whole[:, s * slab : (s + 1) * slab] for s in range(spaces)]
    for s in range(spaces):
        out[:, s] = results[s].reshape(points, 2, rows, slab)


def inverse_y_even(r_ref, *refs):
    tables, out = [ref[...] for ref in refs[:-1]], refs[-1]
    bands, _, rows, slab = r_ref.shape
    half = bands // 2
    for part in range(2):
        total = product(halves(r_ref[:half, part].reshape(half * rows, slab)), tables[:2], TN)
        alternate = product(halves(r_ref[half:, part].reshape(half * rows, slab)), tables[2:], TN)
        out[part] = jnp.concatenate([total + alternate, total - alternate], axis=-1)


def inverse_y_odd(r_ref, even_ref, *refs):
    tables, out = [ref[...] for ref in refs[:-1]], refs[-1]
    bands, _, rows, slab = r_ref.shape
    width = even_ref.shape[-1]
    for part in range(2):
        mixed = product(halves(r_ref[:, part].reshape(bands * rows, slab)), tables, TN)
        out[part, :, :width] = even_ref[part] + mixed
        flipped = even_ref[part] - mixed
        out[part, :, width:] = flipped


def call(kernel, name, operands, outs, flops, scalars=0, scratch=()):
    space = pl.BlockSpec(memory_space=pltpu.VMEM)
    scalar = pl.BlockSpec(memory_space=pltpu.SMEM)
    shapes = [jax.ShapeDtypeStruct(shape, f32) for shape in outs]
    traffic = sum(math.prod(x.shape) * x.dtype.itemsize for x in operands)
    traffic += sum(4 * math.prod(shape) for shape in outs)
    many = len(outs) > 1
    return pl.pallas_call(
        kernel,
        name=name,
        in_specs=[scalar] * scalars + [space] * (len(operands) - scalars),
        out_specs=[space] * len(outs) if many else space,
        out_shape=shapes if many else shapes[0],
        scratch_shapes=[pltpu.VMEM(shape, f32) for shape in scratch],
        cost_estimate=pl.CostEstimate(flops=flops, bytes_accessed=traffic, transcendentals=0),
        compiler_params=pltpu.CompilerParams(vmem_limit_bytes=48 * 2**20),
    )(*operands)


def on_device(residual, counts):
    slab, length_y = residual.shape[2:]
    blocks, points, spaces = (lax.axis_size(name) for name in ("block", "point", "space"))
    length_x = slab * spaces
    group = ("point", "space")
    bands = points * spaces
    rows = length_y // (2 * bands)
    table_x, even_y = (cas_tables(length) for length in (length_x, length_y))
    odd_y, even_y = even_y[4:], even_y[:4]

    shifts = [lax.ppermute(counts, "point", [(i, (i + d) % points) for i in range(points)]) for d in range(1, points)]
    near = [counts] + shifts
    rows_total = 2 * slab

    sent = []
    for odd, tables in enumerate((even_y, odd_y)):
        sent.append(
            call(
                functools.partial(forward_y, bool(odd)),
                "forward_y_%d" % odd,
                [residual[0], *tables],
                [(bands, 2, rows, slab)],
                3 * 2 * rows_total * (length_y // 2) * (length_y // (2 if odd else 4)),
            )
        )
    sent[0], *near = lax.optimization_barrier((sent[0], *near))
    solved = []
    for odd in range(2):
        arrived = lax.all_to_all(sent[odd], group, split_axis=0, concat_axis=0, tiled=True)
        arrived = arrived.reshape(points, spaces, 2, rows, slab)
        spectra, last = call(
            functools.partial(forward_x, odd, length_y, points),
            "forward_x_%d" % odd,
            [*near, arrived, *table_x],
            [(points, 2, rows, length_x), (2, rows, length_x)],
            6 * 2 * rows * points * length_x * length_x // 2,
            scalars=points,
        )
        carry = lax.ppermute(last, "block", [(b, b + 1) for b in range(blocks - 1)])
        if blocks > 2:
            total = sum(near)[0].astype(f32) * (phase_rate / (2.0 * math.pi))
            span = lax.ppermute(total, "block", [(b, b + 1) for b in range(blocks - 1)])
            modulus = modulus_at(place(odd, rows, length_y)[0], (rows, length_x), length_x, length_y)
            reach = 1
            while reach < blocks - 1:
                steps = [(b, b + reach) for b in range(blocks - reach)]
                further = lax.ppermute(carry, "block", steps)
                cosine, sine = turn(span * modulus)
                carry = carry + jnp.stack(
                    [
                        cosine * further[0] + sine * further[1],
                        cosine * further[1] - sine * further[0],
                    ]
                )
                span = span + lax.ppermute(span, "block", steps)
                reach *= 2
        back = call(
            functools.partial(finish_x, odd, length_y, points),
            "finish_x_%d" % odd,
            [*near, spectra, carry, *table_x],
            [(points, spaces, 2, rows, slab)],
            6 * 2 * rows * points * length_x * length_x // 2,
            scalars=points,
            scratch=[(points, 2, rows, length_x)],
        )
        back = back.reshape(bands, 2, rows, slab)
        solved.append(lax.all_to_all(back, group, split_axis=0, concat_axis=0, tiled=True))
    flops = 3 * 2 * rows_total * (length_y // 2) * (length_y // 4)
    even = call(inverse_y_even, "inverse_y_0", [solved[0], *even_y], [(2, slab, length_y // 2)], flops)
    fields = call(inverse_y_odd, "inverse_y_1", [solved[1], even, *odd_y], [(2, slab, length_y)], 2 * flops)
    return fields[None]


def solution(mesh):
    times, spaces = mesh.shape["tm"], mesh.shape["space"]
    points = 4 if times % 4 == 0 else 1
    inner = Mesh(mesh.devices.reshape(times // points, points, spaces), ("block", "point", "space"))
    when = ("block", "point")
    return jax.shard_map(
        on_device,
        mesh=inner,
        in_specs=(P(when, None, "space", None), P(when)),
        out_specs=P(when, None, "space", None),
        check_vma=False,
    )
```

```python
import functools
import math

import jax
import jax.numpy as jnp
import numpy as np
from jax import lax
from jax.experimental import pallas as pl
from jax.experimental.pallas import tpu as pltpu
from jax.sharding import Mesh
from jax.sharding import PartitionSpec as P


phase_rate = 0.004
f32 = jnp.float32
bf16 = jnp.bfloat16
NN = (((1,), (0,)), ((), ()))
NT = (((1,), (1,)), ((), ()))
TN = (((0,), (0,)), ((), ()))
SIN = (3.14159274, -5.1677103, 2.55007744, -0.598291218, 0.0776574388)
COS = (1.0, -4.93480206, 4.05870914, -1.335212, 0.23493728, -0.0243962663)


def cas_tables(length):
    quarter = length // 4
    m = np.arange(quarter, dtype=np.int64)
    j = np.arange(quarter, dtype=np.int64)

    def cas(k, sign=1):
        angle = sign * 2.0 * np.pi * ((k[:, None] * j[None, :]) % length) / length
        return np.cos(angle) + np.sin(angle)

    odd = np.block(
        [
            [cas(4 * m + 1), cas(4 * m + 1, -1)],
            [cas(4 * m + 3), -cas(4 * m + 3, -1)],
        ]
    )
    tables = []
    for table in (cas(4 * m), cas(4 * m + 2), odd):
        table = table.astype(np.float32)
        high = table.astype(jnp.bfloat16)
        low = (table - high.astype(np.float32)).astype(jnp.bfloat16)
        tables += [high, low]
    return tables


def halves(value):
    high = value.astype(bf16)
    return high, (value - high.astype(f32)).astype(bf16)


def product(left, right, form):
    dot = functools.partial(lax.dot_general, dimension_numbers=form, preferred_element_type=f32)
    return dot(left[0], right[0]) + dot(left[0], right[1]) + dot(left[1], right[0])


def fold(parts):
    even, cross = parts[0] + parts[2], parts[1] + parts[3]
    return even + cross, even - cross


def fold_odd(parts):
    return jnp.concatenate([parts[0] - parts[2], parts[1] - parts[3]], axis=-1)


def signed_wave(indices, length):
    return jnp.where(indices < length // 2, indices, indices - length).astype(f32)


def wave_at(spot, length):
    quarter = length // 4
    block = spot // quarter
    return 4 * (spot % quarter) + jnp.where(block == 1, 2, jnp.where(block == 2, 1, block))


def modulus_at(start, start_x, shape, length_x, length_y):
    place_y = start + lax.broadcasted_iota(jnp.int32, shape, 0)
    place_x = start_x + lax.broadcasted_iota(jnp.int32, shape, 1)
    wave_y = signed_wave(wave_at(place_y, length_y), length_y)
    wave_x = signed_wave(wave_at(place_x, length_x), length_x)
    return jnp.sqrt(wave_x * wave_x + wave_y * wave_y)


def turn(angle):
    part = angle - jnp.round(angle)
    square = part * part
    sine = jnp.full_like(square, SIN[-1])
    for factor in SIN[-2::-1]:
        sine = sine * square + factor
    sine = sine * part
    cosine = jnp.full_like(square, COS[-1])
    for factor in COS[-2::-1]:
        cosine = cosine * square + factor
    return 1.0 - 2.0 * sine * sine, 2.0 * sine * cosine


def place(odd, rows, length_y):
    point = lax.axis_index("point")
    band = point * lax.axis_size("space") + lax.axis_index("space")
    return odd * (length_y // 2) + band * rows, point


def rate_of(n, point, count_refs):
    points = len(count_refs)
    shift = lax.rem(point + points - n, points)
    count = count_refs[0][0]
    for d in range(1, points):
        count = jnp.where(shift == d, count_refs[d][0], count)
    return count.astype(f32) * (phase_rate / (2.0 * math.pi))


def copy_in(pairs, sems):
    copies = [pltpu.make_async_copy(source, target, sems.at[i]) for i, (source, target) in enumerate(pairs)]
    for copy in copies:
        copy.start()
    return copies


def copy_out(copies, source, target, sem):
    copies.append(pltpu.make_async_copy(source, target, sem))
    copies[-1].start()


def wait_all(copies):
    for copy in copies:
        copy.wait()


def forward_y(odd, x_hbm, *refs):
    number = (len(refs) - 5) // 2
    tables_hbm, (out_hbm, x_ref, out), refs = refs[:number], refs[number : number + 3], refs[number + 3 :]
    table_refs, (sems, out_sems) = refs[:number], refs[number:]
    pairs = [(x_hbm.at[0], x_ref.at[0])] + list(zip(tables_hbm, table_refs)) + [(x_hbm.at[1], x_ref.at[1])]
    copies = copy_in(pairs, sems)
    wait_all(copies[:-1])
    tables = [ref[...] for ref in table_refs]
    quarter = x_ref.shape[-1] // 4
    _, bands, rows, slab = out.shape
    stores = []
    for part in range(2):
        if part:
            copies[-1].wait()
        pieces = [x_ref[part, :, q * quarter : (q + 1) * quarter] for q in range(4)]
        if odd:
            result = product(tables, halves(fold_odd(pieces)), NT)
            out[part] = result.reshape(bands, rows, slab)
        else:
            total, alternate = fold(pieces)
            half = bands // 2
            out[part, :half] = product(tables[:2], halves(total), NT).reshape(half, rows, slab)
            out[part, half:] = product(tables[2:], halves(alternate), NT).reshape(half, rows, slab)
        copy_out(stores, out.at[part], out_hbm.at[:, part], out_sems.at[part])
    wait_all(stores)


def rotations(odd, length_x, length_y, points, *refs):
    count_refs, (out_hbm, out, sems) = refs[:points], refs[points:]
    _, _, _, rows, quarter = out.shape
    block = math.gcd(rows, 8)
    start, point = place(odd, rows, length_y)
    rates = [rate_of(n, point, count_refs) for n in range(points)]
    stores = []
    for q in range(4):

        def step(index, _):
            here = pl.ds(pl.multiple_of(index * block, block), block)
            modulus = modulus_at(start + index * block, q * quarter, (block, quarter), length_x, length_y)
            for n in range(points):
                out[q, 0, n, here, :], out[q, 1, n, here, :] = turn(rates[n] * modulus)
            return 0

        lax.fori_loop(0, rows // block, step, 0)
        copy_out(stores, out.at[q], out_hbm.at[q], sems.at[q])
    wait_all(stores)


def forward_x(r_ref, turns_hbm, *refs):
    tables, refs = [ref[...] for ref in refs[:-6]], refs[-6:]
    spectra_hbm, last, turns, spectra, sems, out_sems = refs
    points, spaces, _, rows, slab = r_ref.shape
    quarter = spaces * slab // 4
    count = points * 2 * rows
    copies = copy_in([(turns_hbm.at[q], turns.at[q]) for q in range(4)], sems)
    pieces = [r_ref[:, s].reshape(count, slab) for s in range(spaces)]
    if spaces != 4:
        whole = jnp.concatenate(pieces, axis=-1)
        pieces = [whole[:, q * quarter : (q + 1) * quarter] for q in range(4)]
    total, alternate = fold(pieces)
    stores = []

    def finish(q, result):
        result = result.reshape(points, 2, rows, quarter)
        spectra[q] = result
        copy_out(stores, spectra.at[q], spectra_hbm.at[q], out_sems.at[q])
        copies[q].wait()
        first, second = result[0, 0], result[0, 1]
        for n in range(1, points):
            cosine, sine = turns[q, 0, n], turns[q, 1, n]
            first, second = (
                cosine * first + sine * second + result[n, 0],
                cosine * second - sine * first + result[n, 1],
            )
        here = slice(q * quarter, (q + 1) * quarter)
        last[0, :, here] = first
        last[1, :, here] = second

    finish(0, product(halves(total), tables[:2], NT))
    finish(1, product(halves(alternate), tables[2:4], NT))
    mixed = product(halves(fold_odd(pieces)), tables[4:], NT)
    finish(2, mixed[:, :quarter])
    finish(3, mixed[:, quarter:])
    wait_all(stores)


def finish_x(scaling, spectra_hbm, carry, turns_hbm, *refs):
    tables, refs = [ref[...] for ref in refs[:-7]], refs[-7:]
    out_hbm, out, spectra, turns, states, sems, out_sems = refs
    spaces, points, _, rows, slab = out.shape
    quarter = spaces * slab // 4
    count = points * 2 * rows
    pairs = []
    for q in range(4):
        pairs += [(spectra_hbm.at[q], spectra.at[q]), (turns_hbm.at[q], turns.at[q])]
    copies = copy_in(pairs, sems)
    for q in range(4):
        wait_all(copies[2 * q : 2 * q + 2])
        here = slice(q * quarter, (q + 1) * quarter)
        first, second = carry[0, :, here], carry[1, :, here]
        for n in range(points):
            cosine, sine = turns[q, 0, n], turns[q, 1, n]
            first, second = (
                cosine * first + sine * second + spectra[q, n, 0],
                cosine * second - sine * first + spectra[q, n, 1],
            )
            states[n, 0, :, here] = first * scaling
            states[n, 1, :, here] = second * scaling
    total = product(halves(states[..., :quarter].reshape(count, quarter)), tables[:2], NN)
    alternate = product(halves(states[..., quarter : 2 * quarter].reshape(count, quarter)), tables[2:4], NN)
    mixed = product(halves(states[..., 2 * quarter :].reshape(count, 2 * quarter)), tables[4:], NN)
    plus, minus = total + alternate, total - alternate
    straight, crossed = mixed[:, :quarter], mixed[:, quarter:]
    results = [plus + straight, minus + crossed, plus - straight, minus - crossed]
    if spaces != 4:
        whole = jnp.concatenate(results, axis=-1)
        results = [whole[:, s * slab : (s + 1) * slab] for s in range(spaces)]
    stores = []
    for s in range(spaces):
        out[s] = results[s].reshape(points, 2, rows, slab)
        copy_out(stores, out.at[s], out_hbm.at[:, s], out_sems.at[s])
    wait_all(stores)


def inverse_y_even(r_hbm, *refs):
    tables, (out_hbm, r_ref, out, in_sems, sems) = [ref[...] for ref in refs[:-5]], refs[-5:]
    wait_all(copy_in([(r_hbm, r_ref)], in_sems))
    bands, _, rows, slab = r_ref.shape
    half = bands // 2
    stores = []
    for part in range(2):
        total = product(halves(r_ref[:half, part].reshape(half * rows, slab)), tables[:2], TN)
        alternate = product(halves(r_ref[half:, part].reshape(half * rows, slab)), tables[2:], TN)
        out[part] = jnp.concatenate([total + alternate, total - alternate], axis=-1)
        copy_out(stores, out.at[part], out_hbm.at[part], sems.at[part])
    wait_all(stores)


def inverse_y_odd(r_ref, even_hbm, *refs):
    tables, (out_hbm, even, out, sems, out_sems) = [ref[...] for ref in refs[:-5]], refs[-5:]
    bands, _, rows, slab = r_ref.shape
    width = even.shape[-1]
    copies = copy_in([(even_hbm.at[part], even.at[part]) for part in range(2)], sems)
    stores = []
    for part in range(2):
        mixed = product(halves(r_ref[:, part].reshape(bands * rows, slab)), tables, TN)
        copies[part].wait()
        out[part, :, :width] = even[part] + mixed
        out[part, :, width:] = even[part] - mixed
        copy_out(stores, out.at[part], out_hbm.at[part], out_sems.at[part])
    wait_all(stores)


def call(kernel, operands, outs, flops, spaces, out_spaces, scratch=(), limit=20):
    shapes = [space(shape, f32) for shape, space in zip(outs, out_spaces)]
    traffic = sum(math.prod(x.shape) * x.dtype.itemsize for x in operands)
    traffic += sum(4 * math.prod(shape) for shape in outs)
    many = len(outs) > 1
    specs = [pl.BlockSpec(memory_space=space) for space in out_spaces]
    operands = [pltpu.with_memory_space_constraint(x, s) if s == pltpu.HBM else x for x, s in zip(operands, spaces)]
    return pl.pallas_call(
        kernel,
        in_specs=[pl.BlockSpec(memory_space=space) for space in spaces],
        out_specs=specs if many else specs[0],
        out_shape=shapes if many else shapes[0],
        scratch_shapes=list(scratch),
        cost_estimate=pl.CostEstimate(flops=flops, bytes_accessed=traffic, transcendentals=0),
        compiler_params=pltpu.CompilerParams(vmem_limit_bytes=limit * 2**20),
    )(*operands)


def on_device(residual, counts):
    slab, length_y = residual.shape[2:]
    blocks, points, spaces = (lax.axis_size(name) for name in ("block", "point", "space"))
    length_x = slab * spaces
    group = ("point", "space")
    bands = points * spaces
    rows = length_y // (2 * bands)
    quarter = length_x // 4
    table_x, tables_y = (cas_tables(length) for length in (length_x, length_y))
    tables_y = (tables_y[:4], tables_y[4:])
    near = [counts]
    for d in range(1, points):
        near.append(lax.ppermute(counts, "point", [(i, (i + d) % points) for i in range(points)]))
    flops_y = [3 * 4 * slab * (length_y // 2) * (length_y // wide) for wide in (4, 2)]
    flops_x = 3 * 4 * rows * points * length_x * 3 * length_x // 8
    vmem, smem, hbm, sems = pltpu.VMEM, pltpu.SMEM, pltpu.HBM, pltpu.SemaphoreType.DMA
    spectra_shape = (4, points, 2, rows, quarter)
    turns_shape = (4, 2, points, rows, quarter)

    sent = []
    for odd in range(2):
        tables = tables_y[odd]
        sent.append(
            call(
                functools.partial(forward_y, odd),
                [residual[0], *tables],
                [(bands, 2, rows, slab)],
                flops_y[odd],
                [hbm] * (1 + len(tables)),
                [hbm],
                scratch=[
                    vmem(residual.shape[1:], f32),
                    vmem((2, bands, rows, slab), f32),
                    *[vmem(table.shape, bf16) for table in tables],
                    sems((2 + len(tables),)),
                    sems((2,)),
                ],
            )
        )
    sent[0], *near = lax.optimization_barrier((sent[0], *near))
    turns = [
        call(
            functools.partial(rotations, odd, length_x, length_y, points),
            near,
            [turns_shape],
            40 * points * rows * length_x,
            [smem] * points,
            [hbm],
            scratch=[vmem(turns_shape, f32), sems((4,))],
        )
        for odd in range(2)
    ]
    spectra, carry = [None] * 2, [None] * 2
    for odd in range(2):
        arrived = lax.all_to_all(sent[odd], group, split_axis=0, concat_axis=0, tiled=True)
        spectra[odd], last = call(
            forward_x,
            [arrived.reshape(points, spaces, 2, rows, slab), turns[odd], *table_x],
            [spectra_shape, (2, rows, length_x)],
            flops_x,
            [vmem, hbm] + [vmem] * len(table_x),
            [hbm, vmem],
            scratch=[
                vmem(turns_shape, f32),
                vmem(spectra_shape, f32),
                sems((4,)),
                sems((4,)),
            ],
        )
        carry[odd] = lax.ppermute(last, "block", [(b, b + 1) for b in range(blocks - 1)])
        if blocks > 2:
            total = sum(near)[0].astype(f32) * (phase_rate / (2.0 * math.pi))
            span = lax.ppermute(total, "block", [(b, b + 1) for b in range(blocks - 1)])
            modulus = modulus_at(place(odd, rows, length_y)[0], 0, (rows, length_x), length_x, length_y)
            reach = 1
            while reach < blocks - 1:
                steps = [(b, b + reach) for b in range(blocks - reach)]
                further = lax.ppermute(carry[odd], "block", steps)
                cosine, sine = turn(span * modulus)
                carry[odd] = carry[odd] + jnp.stack(
                    [
                        cosine * further[0] + sine * further[1],
                        cosine * further[1] - sine * further[0],
                    ]
                )
                span = span + lax.ppermute(span, "block", steps)
                reach *= 2
    carry[0], spectra[1] = lax.optimization_barrier((carry[0], spectra[1]))
    solved = []
    for odd in range(2):
        back = call(
            functools.partial(finish_x, 1.0 / (length_x * length_y)),
            [spectra[odd], carry[odd], turns[odd], *table_x],
            [(points, spaces, 2, rows, slab)],
            flops_x,
            [hbm, vmem, hbm] + [vmem] * len(table_x),
            [hbm],
            scratch=[
                vmem((spaces, points, 2, rows, slab), f32),
                vmem(spectra_shape, f32),
                vmem(turns_shape, f32),
                vmem((points, 2, rows, length_x), f32),
                sems((8,)),
                sems((spaces,)),
            ],
        )
        back = back.reshape(bands, 2, rows, slab)
        solved.append(lax.all_to_all(back, group, split_axis=0, concat_axis=0, tiled=True))
    half = (2, slab, length_y // 2)
    even = call(
        inverse_y_even,
        [solved[0], *tables_y[0]],
        [half],
        flops_y[0],
        [hbm] + [vmem] * len(tables_y[0]),
        [hbm],
        scratch=[vmem((bands, 2, rows, slab), f32), vmem(half, f32), sems((1,)), sems((2,))],
    )
    fields = call(
        inverse_y_odd,
        [solved[1], even, *tables_y[1]],
        [(2, slab, length_y)],
        flops_y[1],
        [vmem, hbm] + [vmem] * len(tables_y[1]),
        [hbm],
        scratch=[vmem(half, f32), vmem((2, slab, length_y), f32), sems((2,)), sems((2,))],
    )
    return fields[None]


def solution(mesh):
    times, spaces = mesh.shape["tm"], mesh.shape["space"]
    points = 4 if times % 4 == 0 else 1
    inner = Mesh(mesh.devices.reshape(times // points, points, spaces), ("block", "point", "space"))
    when = ("block", "point")
    return jax.shard_map(
        on_device,
        mesh=inner,
        in_specs=(P(when, None, "space", None), P(when)),
        out_specs=P(when, None, "space", None),
        check_vma=False,
    )
```

```python
import functools
import math

import jax
import jax.numpy as jnp
import numpy as np
from jax import lax
from jax.experimental import pallas as pl
from jax.experimental.pallas import tpu as pltpu
from jax.sharding import Mesh
from jax.sharding import PartitionSpec as P


phase_rate = 0.004
f32 = jnp.float32
bf16 = jnp.bfloat16
NN = (((1,), (0,)), ((), ()))
NT = (((1,), (1,)), ((), ()))
TN = (((0,), (0,)), ((), ()))
SIN = (3.14159274, -5.1677103, 2.55007744, -0.598291218, 0.0776574388)
COS = (1.0, -4.93480206, 4.05870914, -1.335212, 0.23493728, -0.0243962663)


def cas_tables(length):
    quarter = length // 4
    m = np.arange(quarter, dtype=np.int64)
    j = np.arange(quarter, dtype=np.int64)

    def cas(k, sign=1):
        angle = sign * 2.0 * np.pi * ((k[:, None] * j[None, :]) % length) / length
        return np.cos(angle) + np.sin(angle)

    odd = np.block(
        [
            [cas(4 * m + 1), cas(4 * m + 1, -1)],
            [cas(4 * m + 3), -cas(4 * m + 3, -1)],
        ]
    )
    tables = []
    for table in (np.concatenate([cas(4 * m), cas(4 * m + 2)], axis=1), odd):
        table = table.astype(np.float32)
        high = table.astype(jnp.bfloat16)
        low = (table - high.astype(np.float32)).astype(jnp.bfloat16)
        tables.append(np.stack([high, low]))
    return tables


def split_tables(even):
    quarter = even.shape[1]
    return tuple((even[0, :, here], even[1, :, here]) for here in (slice(0, quarter), slice(quarter, 2 * quarter)))


def halves(value):
    high = value.astype(bf16)
    return high, (value - high.astype(f32)).astype(bf16)


def product(left, right, form):
    dot = functools.partial(lax.dot_general, dimension_numbers=form, preferred_element_type=f32)
    return dot(left[0], right[0]) + dot(left[0], right[1]) + dot(left[1], right[0])


def fold(parts):
    even, cross = parts[0] + parts[2], parts[1] + parts[3]
    return even + cross, even - cross


def fold_odd(parts):
    return jnp.concatenate([parts[0] - parts[2], parts[1] - parts[3]], axis=-1)


def signed_wave(indices, length):
    return jnp.where(indices < length // 2, indices, indices - length).astype(f32)


def wave_at(spot, length):
    quarter = length // 4
    block = spot // quarter
    return 4 * (spot % quarter) + jnp.where(block == 1, 2, jnp.where(block == 2, 1, block))


def modulus_at(start, start_x, shape, length_x, length_y):
    place_y = start + lax.broadcasted_iota(jnp.int32, shape, 0)
    place_x = start_x + lax.broadcasted_iota(jnp.int32, shape, 1)
    wave_y = signed_wave(wave_at(place_y, length_y), length_y)
    wave_x = signed_wave(wave_at(place_x, length_x), length_x)
    return jnp.sqrt(wave_x * wave_x + wave_y * wave_y)


def turn(angle):
    part = angle - jnp.round(angle)
    square = part * part
    sine = jnp.full_like(square, SIN[-1])
    for factor in SIN[-2::-1]:
        sine = sine * square + factor
    sine = sine * part
    cosine = jnp.full_like(square, COS[-1])
    for factor in COS[-2::-1]:
        cosine = cosine * square + factor
    return 1.0 - 2.0 * sine * sine, 2.0 * sine * cosine


def place(odd, rows, length_y):
    band = lax.axis_index("point") * lax.axis_size("space") + lax.axis_index("space")
    return odd * (length_y // 2) + band * rows


def copy_in(pairs, sems):
    copies = [pltpu.make_async_copy(source, target, sems.at[i]) for i, (source, target) in enumerate(pairs)]
    for copy in copies:
        copy.start()
    return copies


def copy_out(copies, source, target, sem):
    copies.append(pltpu.make_async_copy(source, target, sem))
    copies[-1].start()


def wait_all(copies):
    for copy in copies:
        copy.wait()


def forward_y(odd, count_ref, x_hbm, table_hbm, out_hbm, x_ref, out, table_ref, sems, out_sems):
    pairs = [(x_hbm.at[0], x_ref.at[0]), (table_hbm, table_ref), (x_hbm.at[1], x_ref.at[1])]
    copies = copy_in(pairs, sems)
    bands, height, lanes = out.shape
    slab, length_y = x_ref.shape[1:]
    quarter = length_y // 4
    rows = length_y // (2 * bands)
    tall = slab // lanes * rows
    if not odd:
        out[:, 2 * tall :] = jnp.full((bands, height - 2 * tall, lanes), count_ref[0].astype(f32))
    wait_all(copies[:-1])
    table = table_ref[...]
    stores = []

    def keep(part, first, result):
        reach = result.shape[0] // rows
        for piece in range(slab // lanes):
            start = part * tall + piece * rows
            wanted = result[:, piece * lanes : (piece + 1) * lanes]
            out[first : first + reach, start : start + rows] = wanted.reshape(reach, rows, lanes)

    for part in range(2):
        if part:
            copies[-1].wait()
        pieces = [x_ref[part, :, q * quarter : (q + 1) * quarter] for q in range(4)]
        if odd:
            keep(part, 0, product(table, halves(fold_odd(pieces)), NT))
        else:
            total, alternate = fold(pieces)
            for half, (pair, value) in enumerate(zip(split_tables(table), (total, alternate))):
                keep(part, half * bands // 2, product(pair, halves(value), NT))
        here = pl.ds(part * tall, height - tall if part else tall)
        copy_out(stores, out.at[:, here], out_hbm.at[:, here], out_sems.at[part])
    wait_all(stores)


def rotations(odd, length_x, length_y, out_hbm, out, sems):
    _, _, choices, rows, quarter = out.shape
    block = math.gcd(rows, 8)
    start = place(odd, rows, length_y)
    stores = []
    for q in range(4):

        def step(index, _):
            here = pl.ds(pl.multiple_of(index * block, block), block)
            modulus = modulus_at(start + index * block, q * quarter, (block, quarter), length_x, length_y)
            for n in range(choices):
                rate = phase_rate * (n + 1) / (2.0 * math.pi)
                out[q, 0, n, here, :], out[q, 1, n, here, :] = turn(rate * modulus)
            return 0

        lax.fori_loop(0, rows // block, step, 0)
        copy_out(stores, out.at[q], out_hbm.at[q], sems.at[q])
    wait_all(stores)


def forward_x(odd, *refs):
    refs, (turns, highs, lows, spectra, turn_sems, out_sems) = refs[:-6], refs[-6:]
    if odd:
        count_ref, r_hbm, turns_hbm, even, mixing, spectra_hbm, last, r_ref, sems = refs
        copies = copy_in([(r_hbm.at[n], r_ref.at[n]) for n in range(r_ref.shape[0])], sems)
    else:
        r_ref, turns_hbm, even, mixing, spectra_hbm, last, count_ref = refs
    turn_copies = copy_in([(turns_hbm.at[q], turns.at[q]) for q in (2, 3, 0, 1)], turn_sems)
    points, spaces, _, lanes = r_ref.shape
    _, _, rows, quarter = spectra.shape[1:]
    slab = 4 * quarter // spaces
    tall = slab // lanes * rows
    count = 2 * rows
    if not odd:
        for n in range(points):
            count_ref[n] = jnp.max(r_ref[n, 0, 2 * tall :]).astype(jnp.int32)
    for n in range(points):
        if odd:
            copies[n].wait()
        pieces = []
        for s in range(spaces):
            slices = [r_ref[n, s, start : start + rows] for start in range(0, 2 * tall, rows)]
            wide = slab // lanes
            pieces.append(
                jnp.concatenate(
                    [jnp.concatenate(slices[part * wide : (part + 1) * wide], axis=-1) for part in range(2)],
                    axis=0,
                )
            )
        if spaces != 4:
            whole = jnp.concatenate(pieces, axis=-1)
            pieces = [whole[:, q * quarter : (q + 1) * quarter] for q in range(4)]
        here = slice(n * count, (n + 1) * count)
        columns = [*fold(pieces), pieces[0] - pieces[2], pieces[1] - pieces[3]]
        for q, column in enumerate(columns):
            high, low = halves(column)
            highs[here, q * quarter : (q + 1) * quarter] = high
            lows[here, q * quarter : (q + 1) * quarter] = low
    choice = [jnp.clip(count_ref[n] - 1, 0, turns.shape[2] - 1) for n in range(points)]
    stores = []

    def finish(q, result):
        result = result.reshape(points, 2, rows, quarter)
        spectra[q] = result
        copy_out(stores, spectra.at[q], spectra_hbm.at[q], out_sems.at[q])
        turn_copies[(q + 2) % 4].wait()
        first, second = result[0, 0], result[0, 1]
        for n in range(1, points):
            cosine, sine = turns[q, 0, choice[n]], turns[q, 1, choice[n]]
            first, second = (
                cosine * first + sine * second + result[n, 0],
                cosine * second - sine * first + result[n, 1],
            )
        here = slice(q * quarter, (q + 1) * quarter)
        last[0, :, here] = first
        last[1, :, here] = second

    straight, alternate = split_tables(even[...])
    for first, wide, pair in ((2, 2, mixing[...]), (0, 1, straight), (1, 1, alternate)):
        here = slice(first * quarter, (first + wide) * quarter)
        result = product((highs[:, here], lows[:, here]), pair, NT)
        for q in range(wide):
            finish(first + q, result[:, q * quarter : (q + 1) * quarter])
    wait_all(stores)


def finish_x(scaling, count_ref, spectra, carry, turns, even, mixing, out_hbm, out, states, out_sems):
    spaces, points, _, rows, slab = out.shape
    quarter = spaces * slab // 4
    count = points * 2 * rows
    choice = [jnp.clip(count_ref[n] - 1, 0, turns.shape[2] - 1) for n in range(points)]
    for q in range(4):
        here = slice(q * quarter, (q + 1) * quarter)
        first, second = carry[0, :, here], carry[1, :, here]
        for n in range(points):
            cosine, sine = turns[q, 0, choice[n]], turns[q, 1, choice[n]]
            first, second = (
                cosine * first + sine * second + spectra[q, n, 0],
                cosine * second - sine * first + spectra[q, n, 1],
            )
            states[n, 0, :, here] = first * scaling
            states[n, 1, :, here] = second * scaling
    tables = split_tables(even[...])
    total = product(halves(states[..., :quarter].reshape(count, quarter)), tables[0], NN)
    alternate = product(halves(states[..., quarter : 2 * quarter].reshape(count, quarter)), tables[1], NN)
    mixed = product(halves(states[..., 2 * quarter :].reshape(count, 2 * quarter)), mixing[...], NN)
    plus, minus = total + alternate, total - alternate
    straight, crossed = mixed[:, :quarter], mixed[:, quarter:]
    results = [plus + straight, minus + crossed, plus - straight, minus - crossed]
    if spaces != 4:
        whole = jnp.concatenate(results, axis=-1)
        results = [whole[:, s * slab : (s + 1) * slab] for s in range(spaces)]
    stores = []
    for s in range(spaces):
        out[s] = results[s].reshape(points, 2, rows, slab)
        copy_out(stores, out.at[s], out_hbm.at[:, s], out_sems.at[s])
    wait_all(stores)


def inverse_y_even(r_hbm, table, out_hbm, _, r_ref, out, in_sems, sems):
    tables = split_tables(table[...])
    wait_all(copy_in([(r_hbm, r_ref)], in_sems))
    bands, _, rows, slab = r_ref.shape
    half = bands // 2
    stores = []
    for part in range(2):
        total = product(halves(r_ref[:half, part].reshape(half * rows, slab)), tables[0], TN)
        alternate = product(halves(r_ref[half:, part].reshape(half * rows, slab)), tables[1], TN)
        out[part] = jnp.concatenate([total + alternate, total - alternate], axis=-1)
        copy_out(stores, out.at[part], out_hbm.at[part], sems.at[part])
    wait_all(stores)


def inverse_y_odd(r_ref, even_hbm, table, out_hbm, even, out, sems, out_sems):
    bands, _, rows, slab = r_ref.shape
    width = even.shape[-1]
    copies = copy_in([(even_hbm.at[part], even.at[part]) for part in range(2)], sems)
    stores = []
    step = slab // 2
    for part in range(2):
        for piece in range(2):
            here = slice(piece * step, (piece + 1) * step)
            mixed = product(halves(r_ref[:, part, :, here].reshape(bands * rows, step)), table[...], TN)
            if not piece:
                copies[part].wait()
            out[part, here, :width] = even[part, here] + mixed
            out[part, here, width:] = even[part, here] - mixed
            there = pl.ds(piece * step, step)
            copy_out(stores, out.at[part, there], out_hbm.at[part, there], out_sems.at[2 * part + piece])
    wait_all(stores)


def call(kernel, operands, outs, flops, spaces, out_spaces, scratch=(), limit=20, aliases=None):
    shapes = [space(shape, jnp.int32 if space == pltpu.SMEM else f32) for shape, space in zip(outs, out_spaces)]
    traffic = sum(math.prod(x.shape) * x.dtype.itemsize for x in operands)
    traffic += sum(4 * math.prod(shape) for shape in outs)
    many = len(outs) > 1
    specs = [pl.BlockSpec(memory_space=space) for space in out_spaces]
    operands = [pltpu.with_memory_space_constraint(x, s) if s == pltpu.HBM else x for x, s in zip(operands, spaces)]
    return pl.pallas_call(
        kernel,
        in_specs=[pl.BlockSpec(memory_space=space) for space in spaces],
        out_specs=specs if many else specs[0],
        out_shape=shapes if many else shapes[0],
        scratch_shapes=list(scratch),
        input_output_aliases=aliases or {},
        cost_estimate=pl.CostEstimate(flops=flops, bytes_accessed=traffic, transcendentals=0),
        compiler_params=pltpu.CompilerParams(vmem_limit_bytes=limit * 2**20),
    )(*operands)


def on_device(residual, counts):
    slab, length_y = residual.shape[2:]
    blocks, points, spaces = (lax.axis_size(name) for name in ("block", "point", "space"))
    length_x = slab * spaces
    group = ("point", "space")
    bands = points * spaces
    rows = length_y // (2 * bands)
    quarter = length_x // 4
    table_x, tables_y = (cas_tables(length) for length in (length_x, length_y))
    flops_y = [3 * 4 * slab * (length_y // 2) * (length_y // wide) for wide in (4, 2)]
    flops_x = 3 * 4 * rows * points * length_x * 3 * length_x // 8
    vmem, smem, hbm, sems = pltpu.VMEM, pltpu.SMEM, pltpu.HBM, pltpu.SemaphoreType.DMA
    spectra_shape = (4, points, 2, rows, quarter)
    turns_shape = (4, 2, 4, rows, quarter)

    lanes = math.gcd(slab, 128)
    tall = slab // lanes * rows
    heights = (2 * tall + 8, 2 * tall)

    sent, turns = [], []
    for odd in range(2):
        table = tables_y[odd]
        sent.append(
            call(
                functools.partial(forward_y, odd),
                [counts, residual[0], table],
                [(bands, heights[odd], lanes)],
                flops_y[odd],
                [smem, hbm, hbm],
                [hbm],
                scratch=[
                    vmem(residual.shape[1:], f32),
                    vmem((bands, heights[odd], lanes), f32),
                    vmem(table.shape, bf16),
                    sems((3,)),
                    sems((2,)),
                ],
            )
        )
        turns.append(
            call(
                functools.partial(rotations, odd, length_x, length_y),
                [],
                [turns_shape],
                40 * 4 * rows * length_x,
                [],
                [hbm],
                scratch=[vmem(turns_shape, f32), sems((4,))],
            )
        )
    spectra, carry = [None] * 2, [None] * 2
    for odd in range(2):
        arrived = lax.all_to_all(sent[odd], group, split_axis=0, concat_axis=0, tiled=True)
        if odd:
            arrived, spectra[0], later = lax.optimization_barrier((arrived, spectra[0], turns[0]))
        arrived = arrived.reshape(points, spaces, heights[odd], lanes)
        folded = [vmem((points * 2 * rows, length_x), bf16)] * 2
        results = call(
            functools.partial(forward_x, odd),
            [near, arrived, turns[1], *table_x] if odd else [arrived, turns[0], *table_x],
            [spectra_shape, (2, rows, length_x)] + ([] if odd else [(points,)]),
            flops_x,
            ([smem, pl.ANY] if odd else [vmem]) + [hbm, vmem, vmem],
            [hbm, vmem] + ([] if odd else [smem]),
            scratch=[vmem(arrived.shape, f32), sems((points,))] * odd
            + [vmem(turns_shape, f32), *folded, vmem(spectra_shape, f32), sems((4,)), sems((4,))],
        )
        spectra[odd], last = results[:2]
        if not odd:
            near = results[2]
        carry[odd] = lax.ppermute(last, "block", [(b, b + 1) for b in range(blocks - 1)])
        if blocks > 2:
            total = jnp.sum(near).astype(f32) * (phase_rate / (2.0 * math.pi))
            span = lax.ppermute(total, "block", [(b, b + 1) for b in range(blocks - 1)])
            modulus = modulus_at(place(odd, rows, length_y), 0, (rows, length_x), length_x, length_y)
            reach = 1
            while reach < blocks - 1:
                steps = [(b, b + reach) for b in range(blocks - reach)]
                further = lax.ppermute(carry[odd], "block", steps)
                cosine, sine = turn(span * modulus)
                carry[odd] = carry[odd] + jnp.stack(
                    [
                        cosine * further[0] + sine * further[1],
                        cosine * further[1] - sine * further[0],
                    ]
                )
                span = span + lax.ppermute(span, "block", steps)
                reach *= 2
    carry[0], spectra[1] = lax.optimization_barrier((carry[0], spectra[1]))
    solved = []
    for odd in range(2):
        back = call(
            functools.partial(finish_x, 1.0 / (length_x * length_y)),
            [near, spectra[odd], carry[odd], turns[1] if odd else later, *table_x],
            [(points, spaces, 2, rows, slab)],
            flops_x,
            [smem] + [vmem] * 5,
            [hbm],
            scratch=[
                vmem((spaces, points, 2, rows, slab), f32),
                vmem((points, 2, rows, length_x), f32),
                sems((spaces,)),
            ],
        )
        back = back.reshape(bands, 2, rows, slab)
        solved.append(lax.all_to_all(back, group, split_axis=0, concat_axis=0, tiled=True))
    half = (2, slab, length_y // 2)
    even, _ = call(
        inverse_y_even,
        [solved[0], tables_y[0]],
        [half, solved[0].shape],
        flops_y[0],
        [hbm, vmem],
        [hbm, hbm],
        aliases={0: 1},
        scratch=[vmem((bands, 2, rows, slab), f32), vmem(half, f32), sems((1,)), sems((2,))],
    )
    fields = call(
        inverse_y_odd,
        [solved[1], even, tables_y[1]],
        [(2, slab, length_y)],
        flops_y[1],
        [vmem, hbm, vmem],
        [hbm],
        scratch=[vmem(half, f32), vmem((2, slab, length_y), f32), sems((2,)), sems((4,))],
    )
    return fields[None]


def solution(mesh):
    times, spaces = mesh.shape["tm"], mesh.shape["space"]
    points = 4 if times % 4 == 0 else 1
    inner = Mesh(mesh.devices.reshape(times // points, points, spaces), ("block", "point", "space"))
    when = ("block", "point")
    return jax.shard_map(
        on_device,
        mesh=inner,
        in_specs=(P(when, None, "space", None), P(when)),
        out_specs=P(when, None, "space", None),
        check_vma=False,
    )
```

```python
import functools
import math

import jax
import jax.numpy as jnp
import numpy as np
from jax import lax
from jax.experimental import pallas as pl
from jax.experimental.pallas import tpu as pltpu
from jax.sharding import Mesh
from jax.sharding import PartitionSpec as P


phase_rate = 0.004
f32 = jnp.float32
bf16 = jnp.bfloat16
NN = (((1,), (0,)), ((), ()))
NT = (((1,), (1,)), ((), ()))
TN = (((0,), (0,)), ((), ()))
SIN = (3.14159274, -5.1677103, 2.55007744, -0.598291218, 0.0776574388)
COS = (1.0, -4.93480206, 4.05870914, -1.335212, 0.23493728, -0.0243962663)


def cas_tables(length):
    steps = np.arange(length // 4, dtype=np.int64)

    def cas(k):
        angle = 2.0 * np.pi * ((k[:, None] * steps[None, :]) % length) / length
        return np.cos(angle) + np.sin(angle)

    tables = []
    for pair in ((4 * steps, 4 * steps + 2), (4 * steps + 1, -4 * steps - 1)):
        table = np.stack([cas(k) for k in pair]).astype(np.float32)
        high = table.astype(jnp.bfloat16)
        low = (table - high.astype(np.float32)).astype(jnp.bfloat16)
        tables.append(np.stack([high, low], axis=1))
    return tables


def halves(value):
    high = value.astype(bf16)
    return high, (value - high.astype(f32)).astype(bf16)


def product(left, right, form):
    dot = functools.partial(lax.dot_general, dimension_numbers=form, preferred_element_type=f32)
    return dot(left[0], right[0]) + dot(left[0], right[1]) + dot(left[1], right[0])


def fold(parts):
    even, cross = parts[0] + parts[2], parts[1] + parts[3]
    return even + cross, even - cross


def mix(first, second, table, form):
    plain, turned = table[0], table[1]
    return (
        product(first, plain, form) + product(second, turned, form),
        product(first, turned, form) - product(second, plain, form),
    )


def signed_wave(indices, length):
    return jnp.where(indices < length // 2, indices, indices - length).astype(f32)


def wave_at(spot, length):
    quarter = length // 4
    block = spot // quarter
    wave = 4 * (spot % quarter) + jnp.where(block == 1, 2, jnp.where(block == 0, 0, 1))
    return jnp.where(block == 3, length - wave, wave)


def modulus_at(start, start_x, shape, length_x, length_y):
    place_y = start + lax.broadcasted_iota(jnp.int32, shape, 0)
    place_x = start_x + lax.broadcasted_iota(jnp.int32, shape, 1)
    wave_y = signed_wave(wave_at(place_y, length_y), length_y)
    wave_x = signed_wave(wave_at(place_x, length_x), length_x)
    return jnp.sqrt(wave_x * wave_x + wave_y * wave_y)


def turn(angle):
    part = angle - jnp.round(angle)
    square = part * part
    sine = jnp.full_like(square, SIN[-1])
    for factor in SIN[-2::-1]:
        sine = sine * square + factor
    sine = sine * part
    cosine = jnp.full_like(square, COS[-1])
    for factor in COS[-2::-1]:
        cosine = cosine * square + factor
    return 1.0 - 2.0 * sine * sine, 2.0 * sine * cosine


def place(odd, rows, length_y):
    band = lax.axis_index("point") * lax.axis_size("space") + lax.axis_index("space")
    return odd * (length_y // 2) + band * rows


def copy_in(pairs, sems):
    copies = [pltpu.make_async_copy(source, target, sems.at[i]) for i, (source, target) in enumerate(pairs)]
    for copy in copies:
        copy.start()
    return copies


def copy_out(copies, source, target, sem):
    copies.append(pltpu.make_async_copy(source, target, sem))
    copies[-1].start()


def wait_all(copies):
    for copy in copies:
        copy.wait()


def forward_y(odd, count_ref, x_hbm, table_hbm, out_hbm, x_ref, out, table_ref, sems, out_sems):
    pairs = [(x_hbm.at[0], x_ref.at[0]), (table_hbm, table_ref), (x_hbm.at[1], x_ref.at[1])]
    copies = copy_in(pairs, sems)
    bands, height, lanes = out.shape
    slab, length_y = x_ref.shape[1:]
    quarter = length_y // 4
    rows = length_y // (2 * bands)
    tall = slab // lanes * rows
    wait_all(copies[:-1])
    if not odd:
        out[:, 2 * tall :] = jnp.full((bands, height - 2 * tall, lanes), count_ref[0].astype(f32))
    table = table_ref[...]
    stores = []

    def keep(part, first, result):
        reach = result.shape[0] // rows
        for piece in range(slab // lanes):
            start = part * tall + piece * rows
            wanted = result[:, piece * lanes : (piece + 1) * lanes]
            out[first : first + reach, start : start + rows] = wanted.reshape(reach, rows, lanes)

    for part in range(2):
        if part:
            copies[-1].wait()
        pieces = [x_ref[part, :, q * quarter : (q + 1) * quarter] for q in range(4)]
        if odd:
            first, second = halves(pieces[0] - pieces[2]), halves(pieces[1] - pieces[3])
            plain, turned = table[0], table[1]
            keep(part, 0, product(plain, first, NT) + product(turned, second, NT))
            keep(part, bands // 2, product(turned, first, NT) - product(plain, second, NT))
        else:
            for half, value in enumerate(fold(pieces)):
                keep(part, half * bands // 2, product(table[half], halves(value), NT))
        here = pl.ds(part * tall, height - tall if part else tall)
        copy_out(stores, out.at[:, here], out_hbm.at[:, here], out_sems.at[part])
    wait_all(stores)


def rotations(odd, length_x, length_y, out_hbm, out, sems):
    _, _, choices, rows, quarter = out.shape
    block = math.gcd(rows, 8)
    start = place(odd, rows, length_y)
    stores = []
    for q in range(3):

        def step(index, _):
            here = pl.ds(pl.multiple_of(index * block, block), block)
            modulus = modulus_at(start + index * block, q * quarter, (block, quarter), length_x, length_y)
            for n in range(choices):
                rate = phase_rate * (n + 1) / (2.0 * math.pi)
                out[q, 0, n, here, :], out[q, 1, n, here, :] = turn(rate * modulus)
            return 0

        lax.fori_loop(0, rows // block, step, 0)
        copy_out(stores, out.at[q], out_hbm.at[q], sems.at[q])
    wait_all(stores)


def forward_x(odd, *refs):
    refs, (turns, highs, lows, spectra, turn_sem, out_sems) = refs[:-6], refs[-6:]
    if odd:
        count_ref, r_ref, turns_hbm, even, mixing, spectra_hbm, last = refs
    else:
        r_ref, turns_hbm, even, mixing, spectra_hbm, last, count_ref = refs
    points, spaces, _, lanes = r_ref.shape
    _, _, rows, quarter = spectra.shape[1:]
    slab = 4 * quarter // spaces
    wide = slab // lanes
    tall = wide * rows
    count = 2 * rows
    turn_copy = pltpu.make_async_copy(turns_hbm, turns, turn_sem.at[0])
    turn_copy.start()
    if not odd:
        for n in range(points):
            count_ref[n] = jnp.max(r_ref[n, 0, 2 * tall :]).astype(jnp.int32)

    def gather(n, _):
        pieces = []
        for s in range(spaces):
            slices = [r_ref[n, s, start : start + rows] for start in range(0, 2 * tall, rows)]
            parts = [jnp.concatenate(slices[part * wide : (part + 1) * wide], axis=-1) for part in range(2)]
            pieces.append(jnp.concatenate(parts, axis=0))
        if spaces != 4:
            whole = jnp.concatenate(pieces, axis=-1)
            pieces = [whole[:, q * quarter : (q + 1) * quarter] for q in range(4)]
        here = pl.ds(pl.multiple_of(n * count, count), count)
        columns = [*fold(pieces), pieces[0] - pieces[2], pieces[1] - pieces[3]]
        for q, column in enumerate(columns):
            highs[q, here], lows[q, here] = halves(column)
        return 0

    lax.fori_loop(0, points, gather, 0)
    folded = [(highs[q], lows[q]) for q in range(4)]
    choice = [jnp.clip(count_ref[n] - 1, 0, turns.shape[2] - 1) for n in range(points)]
    stores = []

    def keep(q, result):
        spectra[q] = result.reshape(points, 2, rows, quarter)
        copy_out(stores, spectra.at[q], spectra_hbm.at[q], out_sems.at[q])

    for q, result in zip((2, 3), mix(*folded[2:], mixing, NT)):
        keep(q, result)
    for q in range(2):
        keep(q, product(folded[q], even[q], NT))
    turn_copy.wait()
    for q in (2, 3, 0, 1):
        first, second = spectra[q, 0, 0], spectra[q, 0, 1]
        for n in range(1, points):
            cosine, sine = turns[min(q, 2), 0, choice[n]], turns[min(q, 2), 1, choice[n]]
            first, second = (
                cosine * first + sine * second + spectra[q, n, 0],
                cosine * second - sine * first + spectra[q, n, 1],
            )
        here = slice(q * quarter, (q + 1) * quarter)
        last[0, :, here] = first
        last[1, :, here] = second
    wait_all(stores)


def finish_x(scaling, count_ref, spectra, carry, turns, even, mixing, out_hbm, out, states, out_sems, *scratch):
    if scratch:
        spectra_hbm, turns_hbm, (spectra, turns, sems) = spectra, turns, scratch
        wait_all(copy_in([(turns_hbm, turns), (spectra_hbm, spectra)], sems))
    spaces, points, _, rows, slab = out.shape
    quarter = spaces * slab // 4
    count = points * 2 * rows
    choice = [jnp.clip(count_ref[n] - 1, 0, turns.shape[2] - 1) for n in range(points)]
    for q in range(4):
        first, second = (carry[part, :, q * quarter : (q + 1) * quarter] for part in range(2))
        for n in range(points):
            cosine, sine = turns[min(q, 2), 0, choice[n]], turns[min(q, 2), 1, choice[n]]
            first, second = (
                cosine * first + sine * second + spectra[q, n, 0],
                cosine * second - sine * first + spectra[q, n, 1],
            )
            states[q, n, 0] = first * scaling
            states[q, n, 1] = second * scaling
    waves = [halves(states[q].reshape(count, quarter)) for q in range(4)]
    total, alternate = product(waves[0], even[0], NN), product(waves[1], even[1], NN)
    plus, minus = total + alternate, total - alternate
    straight, crossed = mix(waves[2], waves[3], mixing, NN)
    results = [plus + straight, minus + crossed, plus - straight, minus - crossed]
    if spaces != 4:
        whole = jnp.concatenate(results, axis=-1)
        results = [whole[:, s * slab : (s + 1) * slab] for s in range(spaces)]
    stores = []
    for s in range(spaces):
        out[s] = results[s].reshape(points, 2, rows, slab)
        copy_out(stores, out.at[s], out_hbm.at[:, s], out_sems.at[s])
    wait_all(stores)


def inverse_y_even(r_hbm, table, out_hbm, _, r_ref, out, in_sems, sems):
    wait_all(copy_in([(r_hbm, r_ref)], in_sems))
    bands, _, rows, slab = r_ref.shape
    half = bands // 2
    stores = []
    for part in range(2):
        total = product(halves(r_ref[:half, part].reshape(half * rows, slab)), table[0], TN)
        alternate = product(halves(r_ref[half:, part].reshape(half * rows, slab)), table[1], TN)
        out[part] = jnp.concatenate([total + alternate, total - alternate], axis=-1)
        copy_out(stores, out.at[part], out_hbm.at[part], sems.at[part])
    wait_all(stores)


def inverse_y_odd(r_ref, even_hbm, table, out_hbm, even, out, sems, out_sems):
    bands, _, rows, slab = r_ref.shape
    half = bands // 2
    quarter = even.shape[-1] // 2
    pieces = slab // math.gcd(slab, 128)
    step = slab // pieces
    copies = copy_in([(even_hbm, even)], sems)

    def place_out(index):
        here = (index // pieces, pl.ds(pl.multiple_of(index % pieces * step, step), step))
        return pltpu.make_async_copy(out.at[here], out_hbm.at[here], out_sems.at[index])

    def work(index, _):
        part = index // pieces
        here = pl.ds(pl.multiple_of(index % pieces * step, step), step)
        first = halves(r_ref[:half, part, :, here].reshape(half * rows, step))
        second = halves(r_ref[half:, part, :, here].reshape(half * rows, step))

        @pl.when(index == 0)
        def _():
            wait_all(copies)

        for q, result in enumerate(mix(first, second, table, TN)):
            base = even[part, here, q * quarter : (q + 1) * quarter]
            out[part, here, q * quarter : (q + 1) * quarter] = base + result
            out[part, here, (q + 2) * quarter : (q + 3) * quarter] = base - result
        place_out(index).start()
        return 0

    lax.fori_loop(0, 2 * pieces, work, 0)
    for index in range(2 * pieces):
        place_out(index).wait()


def call(kernel, operands, outs, flops, spaces, out_spaces, scratch=(), limit=20, aliases=None):
    shapes = [space(shape, jnp.int32 if space == pltpu.SMEM else f32) for shape, space in zip(outs, out_spaces)]
    traffic = sum(math.prod(x.shape) * x.dtype.itemsize for x in operands)
    traffic += sum(4 * math.prod(shape) for shape in outs)
    many = len(outs) > 1
    specs = [pl.BlockSpec(memory_space=space) for space in out_spaces]
    operands = [pltpu.with_memory_space_constraint(x, s) if s == pltpu.HBM else x for x, s in zip(operands, spaces)]
    return pl.pallas_call(
        kernel,
        in_specs=[pl.BlockSpec(memory_space=space) for space in spaces],
        out_specs=specs if many else specs[0],
        out_shape=shapes if many else shapes[0],
        scratch_shapes=list(scratch),
        input_output_aliases=aliases or {},
        cost_estimate=pl.CostEstimate(flops=flops, bytes_accessed=traffic, transcendentals=0),
        compiler_params=pltpu.CompilerParams(vmem_limit_bytes=limit * 2**20),
    )(*operands)


def on_device(residual, counts):
    slab, length_y = residual.shape[2:]
    blocks, points, spaces = (lax.axis_size(name) for name in ("block", "point", "space"))
    length_x = slab * spaces
    group = ("point", "space")
    bands = points * spaces
    rows = length_y // (2 * bands)
    quarter = length_x // 4
    table_x, tables_y = (cas_tables(length) for length in (length_x, length_y))
    flops_y = [3 * 4 * slab * (length_y // 2) * (length_y // wide) for wide in (4, 2)]
    flops_x = 3 * 4 * rows * points * length_x * 3 * length_x // 8
    vmem, smem, hbm, sems = pltpu.VMEM, pltpu.SMEM, pltpu.HBM, pltpu.SemaphoreType.DMA
    spectra_shape = (4, points, 2, rows, quarter)
    turns_shape = (3, 2, 4, rows, quarter)

    lanes = math.gcd(slab, 128)
    tall = slab // lanes * rows
    heights = (2 * tall + 8, 2 * tall)

    sent, turns = [], []
    for odd in range(2):
        table = tables_y[odd]
        sent.append(
            call(
                functools.partial(forward_y, odd),
                [counts, residual[0], table],
                [(bands, heights[odd], lanes)],
                flops_y[odd],
                [smem, hbm, hbm],
                [hbm],
                scratch=[
                    vmem(residual.shape[1:], f32),
                    vmem((bands, heights[odd], lanes), f32),
                    vmem(table.shape, bf16),
                    sems((3,)),
                    sems((2,)),
                ],
            )
        )
        turns.append(
            call(
                functools.partial(rotations, odd, length_x, length_y),
                [],
                [turns_shape],
                40 * 4 * rows * length_x,
                [],
                [hbm],
                scratch=[vmem(turns_shape, f32), sems((3,))],
            )
        )
    spectra, carry = [None] * 2, [None] * 2
    for odd in range(2):
        arrived = lax.all_to_all(sent[odd], group, split_axis=0, concat_axis=0, tiled=True)
        if odd:
            arrived, spectra[0], later = lax.optimization_barrier((arrived, spectra[0], turns[0]))
        arrived = arrived.reshape(points, spaces, heights[odd], lanes)
        folded = [vmem((4, points * 2 * rows, quarter), bf16)] * 2
        results = call(
            functools.partial(forward_x, odd),
            [near, arrived, turns[1], *table_x] if odd else [arrived, turns[0], *table_x],
            [spectra_shape, (2, rows, length_x)] + ([] if odd else [(points,)]),
            flops_x,
            [smem] * odd + [vmem, hbm, vmem, vmem],
            [hbm, vmem] + ([] if odd else [smem]),
            scratch=[vmem(turns_shape, f32), *folded, vmem(spectra_shape, f32), sems((1,)), sems((4,))],
        )
        spectra[odd], last = results[:2]
        if not odd:
            near = results[2]
        carry[odd] = lax.ppermute(last, "block", [(b, b + 1) for b in range(blocks - 1)])
        if blocks > 2:
            total = jnp.sum(near).astype(f32) * (phase_rate / (2.0 * math.pi))
            span = lax.ppermute(total, "block", [(b, b + 1) for b in range(blocks - 1)])
            modulus = modulus_at(place(odd, rows, length_y), 0, (rows, length_x), length_x, length_y)
            reach = 1
            while reach < blocks - 1:
                steps = [(b, b + reach) for b in range(blocks - reach)]
                further = lax.ppermute(carry[odd], "block", steps)
                cosine, sine = turn(span * modulus)
                carry[odd] = carry[odd] + jnp.stack(
                    [
                        cosine * further[0] + sine * further[1],
                        cosine * further[1] - sine * further[0],
                    ]
                )
                span = span + lax.ppermute(span, "block", steps)
                reach *= 2
    carry[0], spectra[1] = lax.optimization_barrier((carry[0], spectra[1]))
    solved = []
    for odd in range(2):
        back = call(
            functools.partial(finish_x, 1.0 / (length_x * length_y)),
            [near, spectra[odd], carry[odd], turns[1] if odd else later, *table_x],
            [(points, spaces, 2, rows, slab)],
            flops_x,
            [smem, hbm, vmem, hbm, vmem, vmem] if odd else [smem] + [vmem] * 5,
            [hbm],
            scratch=[
                vmem((spaces, points, 2, rows, slab), f32),
                vmem(spectra_shape, f32),
                sems((spaces,)),
            ]
            + [vmem(spectra_shape, f32), vmem(turns_shape, f32), sems((2,))] * odd,
        )
        back = back.reshape(bands, 2, rows, slab)
        solved.append(lax.all_to_all(back, group, split_axis=0, concat_axis=0, tiled=True))
    half = (2, slab, length_y // 2)
    even, _ = call(
        inverse_y_even,
        [solved[0], tables_y[0]],
        [half, solved[0].shape],
        flops_y[0],
        [hbm, vmem],
        [hbm, hbm],
        aliases={0: 1},
        scratch=[vmem((bands, 2, rows, slab), f32), vmem(half, f32), sems((1,)), sems((2,))],
    )
    fields = call(
        inverse_y_odd,
        [solved[1], even, tables_y[1]],
        [(2, slab, length_y)],
        flops_y[1],
        [vmem, hbm, vmem],
        [hbm],
        scratch=[vmem(half, f32), vmem((2, slab, length_y), f32), sems((1,)), sems((2 * slab // lanes,))],
    )
    return fields[None]


def solution(mesh):
    times, spaces = mesh.shape["tm"], mesh.shape["space"]
    points = 4 if times % 4 == 0 else 1
    inner = Mesh(mesh.devices.reshape(times // points, points, spaces), ("block", "point", "space"))
    when = ("block", "point")
    return jax.shard_map(
        on_device,
        mesh=inner,
        in_specs=(P(when, None, "space", None), P(when)),
        out_specs=P(when, None, "space", None),
        check_vma=False,
    )
```

```python
import functools
import math

import jax
import jax.numpy as jnp
import numpy as np
from jax import lax
from jax.experimental import pallas as pl
from jax.experimental.pallas import tpu as pltpu
from jax.sharding import Mesh
from jax.sharding import PartitionSpec as P


phase_rate = 0.004
f32 = jnp.float32
bf16 = jnp.bfloat16
NN = (((1,), (0,)), ((), ()))
NT = (((1,), (1,)), ((), ()))
TN = (((0,), (0,)), ((), ()))
SIN = (3.14159274, -5.1677103, 2.55007744, -0.598291218, 0.0776574388)
COS = (1.0, -4.93480206, 4.05870914, -1.335212, 0.23493728, -0.0243962663)


def cas_tables(length):
    steps = np.arange(length // 4, dtype=np.int64)

    def cas(k):
        angle = 2.0 * np.pi * ((k[:, None] * steps[None, :]) % length) / length
        return np.cos(angle) + np.sin(angle)

    tables = []
    for pair in ((4 * steps, 4 * steps + 2), (4 * steps + 1, -4 * steps - 1)):
        table = np.stack([cas(k) for k in pair]).astype(np.float32)
        high = table.astype(jnp.bfloat16)
        low = (table - high.astype(np.float32)).astype(jnp.bfloat16)
        tables.append(np.stack([high, low], axis=1))
    return tables


def halves(value):
    high = value.astype(bf16)
    return high, (value - high.astype(f32)).astype(bf16)


def product(left, right, form):
    dot = functools.partial(lax.dot_general, dimension_numbers=form, preferred_element_type=f32)
    return dot(left[0], right[0]) + dot(left[0], right[1]) + dot(left[1], right[0])


def fold(parts):
    even, cross = parts[0] + parts[2], parts[1] + parts[3]
    return even + cross, even - cross


def mix(first, second, table, form):
    plain, turned = table[0], table[1]
    return (
        product(first, plain, form) + product(second, turned, form),
        product(first, turned, form) - product(second, plain, form),
    )


def signed_wave(indices, length):
    return jnp.where(indices < length // 2, indices, indices - length).astype(f32)


def wave_at(spot, length):
    quarter = length // 4
    block = spot // quarter
    wave = 4 * (spot % quarter) + jnp.where(block == 1, 2, jnp.where(block == 0, 0, 1))
    return jnp.where(block == 3, length - wave, wave)


def modulus_at(kind, start, start_x, shape, length_x, length_y):
    place_y = kind * (length_y // 4) + start + lax.broadcasted_iota(jnp.int32, shape, 0)
    place_x = start_x + lax.broadcasted_iota(jnp.int32, shape, 1)
    wave_y = signed_wave(wave_at(place_y, length_y), length_y)
    wave_x = signed_wave(wave_at(place_x, length_x), length_x)
    return jnp.sqrt(wave_x * wave_x + wave_y * wave_y)


def turn(angle):
    part = angle - jnp.round(angle)
    square = part * part
    sine = jnp.full_like(square, SIN[-1])
    for factor in SIN[-2::-1]:
        sine = sine * square + factor
    sine = sine * part
    cosine = jnp.full_like(square, COS[-1])
    for factor in COS[-2::-1]:
        cosine = cosine * square + factor
    return 1.0 - 2.0 * sine * sine, 2.0 * sine * cosine


def own_band():
    return lax.axis_index("point") * lax.axis_size("space") + lax.axis_index("space")


def copy_in(pairs, sems):
    copies = [pltpu.make_async_copy(source, target, sems.at[i]) for i, (source, target) in enumerate(pairs)]
    for copy in copies:
        copy.start()
    return copies


def copy_out(copies, source, target, sem):
    copies.append(pltpu.make_async_copy(source, target, sem))
    copies[-1].start()


def wait_all(copies):
    for copy in copies:
        copy.wait()


def forward_y(count_ref, x_hbm, even_hbm, odd_hbm, out_hbm, x_ref, out, even, mixing, sems, out_sems):
    pairs = [(x_hbm.at[0], x_ref.at[0]), (even_hbm, even), (odd_hbm, mixing), (x_hbm.at[1], x_ref.at[1])]
    copies = copy_in(pairs, sems)
    bands, height, lanes = out.shape
    slab, length_y = x_ref.shape[1:]
    quarter = length_y // 4
    small = quarter // bands
    tall = slab // lanes * 4 * small
    out[:, 2 * tall :] = jnp.full((bands, height - 2 * tall, lanes), count_ref[0].astype(f32))
    wait_all(copies[:-1])
    stores = []
    for part in range(2):
        if part:
            copies[-1].wait()
        pieces = [x_ref[part, :, q * quarter : (q + 1) * quarter] for q in range(4)]
        first, second = halves(pieces[0] - pieces[2]), halves(pieces[1] - pieces[3])
        plain, turned = mixing[0], mixing[1]
        results = [product(even[half], halves(value), NT) for half, value in enumerate(fold(pieces))]
        results.append(product(plain, first, NT) + product(turned, second, NT))
        results.append(product(turned, first, NT) - product(plain, second, NT))
        for kind, result in enumerate(results):
            for piece in range(slab // lanes):
                start = part * tall + (piece * 4 + kind) * small
                wanted = result[:, piece * lanes : (piece + 1) * lanes]
                out[:, start : start + small] = wanted.reshape(bands, small, lanes)
        here = pl.ds(part * tall, height - tall if part else tall)
        copy_out(stores, out.at[:, here], out_hbm.at[:, here], out_sems.at[part])
    wait_all(stores)


def rotations(kinds, length_x, length_y, out_hbm, out, sems):
    _, _, choices, rows, quarter = out.shape
    small = rows // len(kinds)
    block = math.gcd(small, 8)
    start = own_band() * small
    stores = []
    for q in range(3):

        def step(index, _):
            here = pl.ds(pl.multiple_of(index * block, block), block)
            kind, within = kinds[0] + index * block // small, index * block % small
            modulus = modulus_at(kind, start + within, q * quarter, (block, quarter), length_x, length_y)
            for n in range(choices):
                rate = phase_rate * (n + 1) / (2.0 * math.pi)
                out[q, 0, n, here, :], out[q, 1, n, here, :] = turn(rate * modulus)
            return 0

        lax.fori_loop(0, rows // block, step, 0)
        copy_out(stores, out.at[q], out_hbm.at[q], sems.at[q])
    wait_all(stores)


def forward_x(kinds, *refs):
    refs, (turns, highs, lows, spectra, turn_sem, out_sems) = refs[:-6], refs[-6:]
    late = kinds[0] > 0
    if late:
        count_ref, r_ref, turns_hbm, even, mixing, spectra_hbm, last = refs
    else:
        r_ref, turns_hbm, even, mixing, spectra_hbm, last, count_ref = refs
    points, spaces, _, lanes = r_ref.shape
    _, _, rows, quarter = spectra.shape[1:]
    slab = 4 * quarter // spaces
    wide = slab // lanes
    small = rows // len(kinds)
    stride, offset = 4 * small, kinds[0] * small
    tall = wide * stride
    count = 2 * rows
    turn_copy = pltpu.make_async_copy(turns_hbm, turns, turn_sem.at[0])
    turn_copy.start()
    if not late:
        for n in range(points):
            count_ref[n] = jnp.max(r_ref[n, 0, 2 * tall :]).astype(jnp.int32)

    def gather(n, _):
        pieces = []
        for s in range(spaces):
            slices = [r_ref[n, s, start : start + rows] for start in range(offset, 2 * tall, stride)]
            parts = [jnp.concatenate(slices[part * wide : (part + 1) * wide], axis=-1) for part in range(2)]
            pieces.append(jnp.concatenate(parts, axis=0))
        if spaces != 4:
            whole = jnp.concatenate(pieces, axis=-1)
            pieces = [whole[:, q * quarter : (q + 1) * quarter] for q in range(4)]
        here = pl.ds(pl.multiple_of(n * count, count), count)
        columns = [*fold(pieces), pieces[0] - pieces[2], pieces[1] - pieces[3]]
        for q, column in enumerate(columns):
            highs[q, here], lows[q, here] = halves(column)
        return 0

    lax.fori_loop(0, points, gather, 0)
    folded = [(highs[q], lows[q]) for q in range(4)]
    choice = [jnp.clip(count_ref[n] - 1, 0, turns.shape[2] - 1) for n in range(points)]
    stores = []

    def keep(q, result):
        spectra[q] = result.reshape(points, 2, rows, quarter)
        copy_out(stores, spectra.at[q], spectra_hbm.at[q], out_sems.at[q])

    for q, result in zip((2, 3), mix(*folded[2:], mixing, NT)):
        keep(q, result)
    for q in range(2):
        keep(q, product(folded[q], even[q], NT))
    turn_copy.wait()
    for q in (2, 3, 0, 1):
        first, second = spectra[q, 0, 0], spectra[q, 0, 1]
        for n in range(1, points):
            cosine, sine = turns[min(q, 2), 0, choice[n]], turns[min(q, 2), 1, choice[n]]
            first, second = (
                cosine * first + sine * second + spectra[q, n, 0],
                cosine * second - sine * first + spectra[q, n, 1],
            )
        here = slice(q * quarter, (q + 1) * quarter)
        last[0, :, here] = first
        last[1, :, here] = second
    wait_all(stores)


def finish_x(scaling, count_ref, spectra, carry, turns, even, mixing, out_hbm, out, states, out_sems, *scratch):
    if scratch:
        spectra_hbm, turns_hbm, (spectra, turns, sems) = spectra, turns, scratch
        wait_all(copy_in([(turns_hbm, turns), (spectra_hbm, spectra)], sems))
    spaces, points, _, rows, slab = out.shape
    quarter = spaces * slab // 4
    count = points * 2 * rows
    choice = [jnp.clip(count_ref[n] - 1, 0, turns.shape[2] - 1) for n in range(points)]
    for q in range(4):
        first, second = (carry[part, :, q * quarter : (q + 1) * quarter] for part in range(2))
        for n in range(points):
            cosine, sine = turns[min(q, 2), 0, choice[n]], turns[min(q, 2), 1, choice[n]]
            first, second = (
                cosine * first + sine * second + spectra[q, n, 0],
                cosine * second - sine * first + spectra[q, n, 1],
            )
            states[q, n, 0] = first * scaling
            states[q, n, 1] = second * scaling
    waves = [halves(states[q].reshape(count, quarter)) for q in range(4)]
    total, alternate = product(waves[0], even[0], NN), product(waves[1], even[1], NN)
    plus, minus = total + alternate, total - alternate
    straight, crossed = mix(waves[2], waves[3], mixing, NN)
    results = [plus + straight, minus + crossed, plus - straight, minus - crossed]
    if spaces != 4:
        whole = jnp.concatenate(results, axis=-1)
        results = [whole[:, s * slab : (s + 1) * slab] for s in range(spaces)]
    stores = []
    for s in range(spaces):
        out[s] = results[s].reshape(points, 2, rows, slab)
        copy_out(stores, out.at[s], out_hbm.at[:, s], out_sems.at[s])
    wait_all(stores)


def inverse_y_first(r_hbm, even, out_hbm, _, r_ref, out, in_sems, sems):
    wait_all(copy_in([(r_hbm, r_ref)], in_sems))
    bands, _, rows, slab = r_ref.shape
    stores = []
    for part in range(2):
        out[part] = product(halves(r_ref[:, part].reshape(bands * rows, slab)), even[0], TN)
        copy_out(stores, out.at[part], out_hbm.at[part], sems.at[part])
    wait_all(stores)


def inverse_y_rest(r_ref, first_hbm, even, mixing, out_hbm, total, out, sems, out_sems):
    bands, _, rows, slab = r_ref.shape
    small = rows // 3
    quarter = total.shape[-1]
    pieces = slab // math.gcd(slab, 128)
    step = slab // pieces
    copies = copy_in([(first_hbm, total)], sems)
    stores = []
    for part in range(2):
        for piece in range(pieces):
            here = slice(piece * step, (piece + 1) * step)
            waves = [
                halves(r_ref[:, part, kind * small : (kind + 1) * small, here].reshape(bands * small, step))
                for kind in range(3)
            ]
            alternate = product(waves[0], even[1], TN)
            straight, crossed = mix(waves[1], waves[2], mixing, TN)
            if not stores:
                wait_all(copies)
            plus, minus = total[part, here] + alternate, total[part, here] - alternate
            for q, result in enumerate((plus + straight, minus + crossed, plus - straight, minus - crossed)):
                out[part, here, q * quarter : (q + 1) * quarter] = result
            there = pl.ds(piece * step, step)
            copy_out(stores, out.at[part, there], out_hbm.at[part, there], out_sems.at[part * pieces + piece])
    wait_all(stores)


def call(kernel, operands, outs, flops, spaces, out_spaces, scratch=(), limit=20, aliases=None):
    shapes = [space(shape, jnp.int32 if space == pltpu.SMEM else f32) for shape, space in zip(outs, out_spaces)]
    traffic = sum(math.prod(x.shape) * x.dtype.itemsize for x in operands)
    traffic += sum(4 * math.prod(shape) for shape in outs)
    many = len(outs) > 1
    specs = [pl.BlockSpec(memory_space=space) for space in out_spaces]
    operands = [pltpu.with_memory_space_constraint(x, s) if s == pltpu.HBM else x for x, s in zip(operands, spaces)]
    return pl.pallas_call(
        kernel,
        in_specs=[pl.BlockSpec(memory_space=space) for space in spaces],
        out_specs=specs if many else specs[0],
        out_shape=shapes if many else shapes[0],
        scratch_shapes=list(scratch),
        input_output_aliases=aliases or {},
        cost_estimate=pl.CostEstimate(flops=flops, bytes_accessed=traffic, transcendentals=0),
        compiler_params=pltpu.CompilerParams(vmem_limit_bytes=limit * 2**20),
    )(*operands)


def on_device(residual, counts):
    slab, length_y = residual.shape[2:]
    blocks, points, spaces = (lax.axis_size(name) for name in ("block", "point", "space"))
    length_x = slab * spaces
    group = ("point", "space")
    bands = points * spaces
    small = length_y // (4 * bands)
    quarter = length_x // 4
    table_x, table_y = cas_tables(length_x), cas_tables(length_y)
    vmem, smem, hbm, sems = pltpu.VMEM, pltpu.SMEM, pltpu.HBM, pltpu.SemaphoreType.DMA
    lanes = math.gcd(slab, 128)
    height = 8 * (slab // lanes) * small + 8

    def flops_y(parts):
        return 3 * 4 * slab * parts * (length_y // 4) ** 2

    sent = call(
        forward_y,
        [counts, residual[0], *table_y],
        [(bands, height, lanes)],
        flops_y(6),
        [smem, hbm, hbm, hbm],
        [hbm],
        scratch=[
            vmem(residual.shape[1:], f32),
            vmem((bands, height, lanes), f32),
            *[vmem(table.shape, bf16) for table in table_y],
            sems((4,)),
            sems((2,)),
        ],
    )
    arrived = lax.all_to_all(sent, group, split_axis=0, concat_axis=0, tiled=True)
    arrived = arrived.reshape(points, spaces, height, lanes)
    turns, spectra, carry = [], [], []
    shapes = []
    for chunk, kinds in enumerate(CHUNKS):
        rows = len(kinds) * small
        shapes.append(((4, points, 2, rows, quarter), (3, 2, 4, rows, quarter)))
        spectra_shape, turns_shape = shapes[-1]
        flops_x = 3 * 4 * rows * points * 6 * quarter * quarter
        turns.append(
            call(
                functools.partial(rotations, kinds, length_x, length_y),
                [],
                [turns_shape],
                40 * 4 * rows * length_x,
                [],
                [hbm],
                scratch=[vmem(turns_shape, f32), sems((3,))],
            )
        )
        folded = [vmem((4, points * 2 * rows, quarter), bf16)] * 2
        results = call(
            functools.partial(forward_x, kinds),
            ([near] if chunk else []) + [arrived, turns[chunk], *table_x],
            [spectra_shape, (2, rows, length_x)] + ([] if chunk else [(points,)]),
            flops_x,
            [smem] * chunk + [vmem, hbm, vmem, vmem],
            [hbm, vmem] + ([] if chunk else [smem]),
            scratch=[vmem(turns_shape, f32), *folded, vmem(spectra_shape, f32), sems((1,)), sems((4,))],
        )
        spectra.append(results[0])
        last = results[1]
        if not chunk:
            near = results[2]
        carry.append(lax.ppermute(last, "block", [(b, b + 1) for b in range(blocks - 1)]))
        if blocks > 2:
            whole = jnp.sum(near).astype(f32) * (phase_rate / (2.0 * math.pi))
            span = lax.ppermute(whole, "block", [(b, b + 1) for b in range(blocks - 1)])
            start = own_band() * small
            modulus = [modulus_at(kind, start, 0, (small, length_x), length_x, length_y) for kind in kinds]
            modulus = jnp.concatenate(modulus, axis=0)
            reach = 1
            while reach < blocks - 1:
                steps = [(b, b + reach) for b in range(blocks - reach)]
                further = lax.ppermute(carry[chunk], "block", steps)
                cosine, sine = turn(span * modulus)
                carry[chunk] = carry[chunk] + jnp.stack(
                    [
                        cosine * further[0] + sine * further[1],
                        cosine * further[1] - sine * further[0],
                    ]
                )
                span = span + lax.ppermute(span, "block", steps)
                reach *= 2
    carry[0], spectra[1] = lax.optimization_barrier((carry[0], spectra[1]))
    solved = []
    for chunk, kinds in enumerate(CHUNKS):
        rows = len(kinds) * small
        spectra_shape, turns_shape = shapes[chunk]
        back = call(
            functools.partial(finish_x, 1.0 / (length_x * length_y)),
            [near, spectra[chunk], carry[chunk], turns[chunk], *table_x],
            [(points, spaces, 2, rows, slab)],
            3 * 4 * rows * points * 6 * quarter * quarter,
            [smem, hbm, vmem, hbm, vmem, vmem] if chunk else [smem] + [vmem] * 5,
            [hbm],
            scratch=[
                vmem((spaces, points, 2, rows, slab), f32),
                vmem(spectra_shape, f32),
                sems((spaces,)),
            ]
            + [vmem(spectra_shape, f32), vmem(turns_shape, f32), sems((2,))] * chunk,
        )
        back = back.reshape(bands, 2, rows, slab)
        solved.append(lax.all_to_all(back, group, split_axis=0, concat_axis=0, tiled=True))
    part_shape = (2, slab, length_y // 4)
    first, _ = call(
        inverse_y_first,
        [solved[0], table_y[0]],
        [part_shape, solved[0].shape],
        flops_y(1),
        [hbm, vmem],
        [hbm, hbm],
        aliases={0: 1},
        scratch=[vmem(solved[0].shape, f32), vmem(part_shape, f32), sems((1,)), sems((2,))],
    )
    fields = call(
        inverse_y_rest,
        [solved[1], first, *table_y],
        [(2, slab, length_y)],
        flops_y(5),
        [vmem, hbm, vmem, vmem],
        [hbm],
        scratch=[
            vmem(part_shape, f32),
            vmem((2, slab, length_y), f32),
            sems((1,)),
            sems((2 * slab // lanes,)),
        ],
    )
    return fields[None]


CHUNKS = ((0,), (1, 2, 3))


def solution(mesh):
    times, spaces = mesh.shape["tm"], mesh.shape["space"]
    points = 4 if times % 4 == 0 else 1
    inner = Mesh(mesh.devices.reshape(times // points, points, spaces), ("block", "point", "space"))
    when = ("block", "point")
    return jax.shard_map(
        on_device,
        mesh=inner,
        in_specs=(P(when, None, "space", None), P(when)),
        out_specs=P(when, None, "space", None),
        check_vma=False,
    )
```

```python
import functools
import math

import jax
import jax.numpy as jnp
import numpy as np
from jax import lax
from jax.experimental import pallas as pl
from jax.experimental.pallas import tpu as pltpu
from jax.sharding import Mesh
from jax.sharding import PartitionSpec as P


phase_rate = 0.004
f32 = jnp.float32
bf16 = jnp.bfloat16
NN = (((1,), (0,)), ((), ()))
NT = (((1,), (1,)), ((), ()))
TN = (((0,), (0,)), ((), ()))
SIN = (3.14159274, -5.1677103, 2.55007744, -0.598291218, 0.0776574388)
COS = (1.0, -4.93480206, 4.05870914, -1.335212, 0.23493728, -0.0243962663)


def cas_tables(length):
    steps = np.arange(length // 4, dtype=np.int64)

    def cas(k):
        angle = 2.0 * np.pi * ((k[:, None] * steps[None, :]) % length) / length
        return np.cos(angle) + np.sin(angle)

    tables = []
    for pair in ((4 * steps, 4 * steps + 2), (4 * steps + 1, -4 * steps - 1)):
        table = np.stack([cas(k) for k in pair]).astype(np.float32)
        high = table.astype(jnp.bfloat16)
        low = (table - high.astype(np.float32)).astype(jnp.bfloat16)
        tables.append(np.stack([high, low], axis=1))
    return tables


def halves(value):
    high = value.astype(bf16)
    return high, (value - high.astype(f32)).astype(bf16)


def product(left, right, form):
    dot = functools.partial(lax.dot_general, dimension_numbers=form, preferred_element_type=f32)
    return dot(left[0], right[0]) + dot(left[0], right[1]) + dot(left[1], right[0])


def fold(parts):
    even, cross = parts[0] + parts[2], parts[1] + parts[3]
    return even + cross, even - cross


def mix(first, second, table, form):
    plain, turned = table[0], table[1]
    return (
        product(first, plain, form) + product(second, turned, form),
        product(first, turned, form) - product(second, plain, form),
    )


def signed_wave(indices, length):
    return jnp.where(indices < length // 2, indices, indices - length).astype(f32)


def wave_at(spot, length):
    quarter = length // 4
    block = spot // quarter
    wave = 4 * (spot % quarter) + jnp.where(block == 1, 2, jnp.where(block == 0, 0, 1))
    return jnp.where(block == 3, length - wave, wave)


def modulus_at(kind, start, start_x, shape, length_x, length_y):
    place_y = kind * (length_y // 4) + start + lax.broadcasted_iota(jnp.int32, shape, 0)
    place_x = start_x + lax.broadcasted_iota(jnp.int32, shape, 1)
    wave_y = signed_wave(wave_at(place_y, length_y), length_y)
    wave_x = signed_wave(wave_at(place_x, length_x), length_x)
    return jnp.sqrt(wave_x * wave_x + wave_y * wave_y)


def turn(angle):
    part = angle - jnp.round(angle)
    square = part * part
    sine = jnp.full_like(square, SIN[-1])
    for factor in SIN[-2::-1]:
        sine = sine * square + factor
    sine = sine * part
    cosine = jnp.full_like(square, COS[-1])
    for factor in COS[-2::-1]:
        cosine = cosine * square + factor
    return 1.0 - 2.0 * sine * sine, 2.0 * sine * cosine


def own_band():
    return lax.axis_index("point") * lax.axis_size("space") + lax.axis_index("space")


def copy_in(pairs, sems):
    copies = [pltpu.make_async_copy(source, target, sems.at[i]) for i, (source, target) in enumerate(pairs)]
    for copy in copies:
        copy.start()
    return copies


def copy_out(copies, source, target, sem):
    copies.append(pltpu.make_async_copy(source, target, sem))
    copies[-1].start()


def wait_all(copies):
    for copy in copies:
        copy.wait()


def forward_y(kinds, late, count_ref, x_hbm, even_hbm, odd_hbm, out_hbm, x_ref, out, even, mixing, sems, out_sems):
    pairs = [(x_hbm.at[0], x_ref.at[0]), (even_hbm, even), (x_hbm.at[1], x_ref.at[1])]
    if kinds[-1] > 1:
        pairs.insert(1, (odd_hbm, mixing))
    copies = copy_in(pairs, sems)
    bands, height, lanes = out.shape
    slab, length_y = x_ref.shape[1:]
    quarter = length_y // 4
    small = quarter // bands
    tall = slab // lanes * len(kinds) * small
    if not late:
        out[:, 2 * tall :] = jnp.full((bands, height - 2 * tall, lanes), count_ref[0].astype(f32))
    wait_all(copies[:-1])
    stores = []
    for part in range(2):
        if part:
            copies[-1].wait()
        pieces = [x_ref[part, :, q * quarter : (q + 1) * quarter] for q in range(4)]
        results = {}
        for kind, value in enumerate(fold(pieces)):
            if kind in kinds:
                results[kind] = product(even[kind], halves(value), NT)
        if kinds[-1] > 1:
            first, second = halves(pieces[0] - pieces[2]), halves(pieces[1] - pieces[3])
            plain, turned = mixing[0], mixing[1]
            results[2] = product(plain, first, NT) + product(turned, second, NT)
            results[3] = product(turned, first, NT) - product(plain, second, NT)
        for index, kind in enumerate(kinds):
            for piece in range(slab // lanes):
                start = part * tall + (piece * len(kinds) + index) * small
                wanted = results[kind][:, piece * lanes : (piece + 1) * lanes]
                out[:, start : start + small] = wanted.reshape(bands, small, lanes)
        here = pl.ds(part * tall, height - tall if part else tall)
        copy_out(stores, out.at[:, here], out_hbm.at[:, here], out_sems.at[part])
    wait_all(stores)


def rotations(kinds, length_x, length_y, out_hbm, out, sems):
    _, _, choices, rows, quarter = out.shape
    small = rows // len(kinds)
    block = math.gcd(small, 8)
    start = own_band() * small
    stores = []
    for q in range(3):

        def step(index, _):
            here = pl.ds(pl.multiple_of(index * block, block), block)
            kind, within = kinds[0] + index * block // small, index * block % small
            modulus = modulus_at(kind, start + within, q * quarter, (block, quarter), length_x, length_y)
            for n in range(choices):
                rate = phase_rate * (n + 1) / (2.0 * math.pi)
                out[q, 0, n, here, :], out[q, 1, n, here, :] = turn(rate * modulus)
            return 0

        lax.fori_loop(0, rows // block, step, 0)
        copy_out(stores, out.at[q], out_hbm.at[q], sems.at[q])
    wait_all(stores)


def forward_x(late, *refs):
    refs, (turns, highs, lows, spectra, turn_sem, out_sems) = refs[:-6], refs[-6:]
    if late:
        count_ref, r_ref, turns_hbm, even, mixing, spectra_hbm, last = refs
    else:
        r_ref, turns_hbm, even, mixing, spectra_hbm, last, count_ref = refs
    points, spaces, _, lanes = r_ref.shape
    _, _, rows, quarter = spectra.shape[1:]
    slab = 4 * quarter // spaces
    wide = slab // lanes
    tall = wide * rows
    count = 2 * rows
    turn_copy = pltpu.make_async_copy(turns_hbm, turns, turn_sem.at[0])
    turn_copy.start()
    if not late:
        for n in range(points):
            count_ref[n] = jnp.max(r_ref[n, 0, 2 * tall :]).astype(jnp.int32)

    def gather(n, _):
        pieces = []
        for s in range(spaces):
            slices = [r_ref[n, s, start : start + rows] for start in range(0, 2 * tall, rows)]
            parts = [jnp.concatenate(slices[part * wide : (part + 1) * wide], axis=-1) for part in range(2)]
            pieces.append(jnp.concatenate(parts, axis=0))
        if spaces != 4:
            whole = jnp.concatenate(pieces, axis=-1)
            pieces = [whole[:, q * quarter : (q + 1) * quarter] for q in range(4)]
        here = pl.ds(pl.multiple_of(n * count, count), count)
        columns = [*fold(pieces), pieces[0] - pieces[2], pieces[1] - pieces[3]]
        for q, column in enumerate(columns):
            highs[q, here], lows[q, here] = halves(column)
        return 0

    lax.fori_loop(0, points, gather, 0)
    folded = [(highs[q], lows[q]) for q in range(4)]
    choice = [jnp.clip(count_ref[n] - 1, 0, turns.shape[2] - 1) for n in range(points)]
    stores = []

    def keep(q, result):
        spectra[q] = result.reshape(points, 2, rows, quarter)
        copy_out(stores, spectra.at[q], spectra_hbm.at[q], out_sems.at[q])

    for q, result in zip((2, 3), mix(*folded[2:], mixing, NT)):
        keep(q, result)
    for q in range(2):
        keep(q, product(folded[q], even[q], NT))
    turn_copy.wait()
    for q in (2, 3, 0, 1):
        first, second = spectra[q, 0, 0], spectra[q, 0, 1]
        for n in range(1, points):
            cosine, sine = turns[min(q, 2), 0, choice[n]], turns[min(q, 2), 1, choice[n]]
            first, second = (
                cosine * first + sine * second + spectra[q, n, 0],
                cosine * second - sine * first + spectra[q, n, 1],
            )
        here = slice(q * quarter, (q + 1) * quarter)
        last[0, :, here] = first
        last[1, :, here] = second
    wait_all(stores)


def finish_x(scaling, first_row, count_ref, spectra, carry, turns, even, mixing, *refs):
    out_hbm, out, states, out_sems = refs[-4:]
    spaces, points, _, rows, slab = out.shape
    quarter = spaces * slab // 4
    count = points * 2 * rows
    choice = [jnp.clip(count_ref[n] - 1, 0, turns.shape[2] - 1) for n in range(points)]
    for q in range(4):
        first, second = (carry[part, :, q * quarter : (q + 1) * quarter] for part in range(2))
        for n in range(points):
            cosine, sine = turns[min(q, 2), 0, choice[n]], turns[min(q, 2), 1, choice[n]]
            first, second = (
                cosine * first + sine * second + spectra[q, n, 0],
                cosine * second - sine * first + spectra[q, n, 1],
            )
            states[q, n, 0] = first * scaling
            states[q, n, 1] = second * scaling
    waves = [halves(states[q].reshape(count, quarter)) for q in range(4)]
    total, alternate = product(waves[0], even[0], NN), product(waves[1], even[1], NN)
    plus, minus = total + alternate, total - alternate
    straight, crossed = mix(waves[2], waves[3], mixing, NN)
    results = [plus + straight, minus + crossed, plus - straight, minus - crossed]
    if spaces != 4:
        whole = jnp.concatenate(results, axis=-1)
        results = [whole[:, s * slab : (s + 1) * slab] for s in range(spaces)]
    stores = []
    for s in range(spaces):
        out[s] = results[s].reshape(points, 2, rows, slab)
        there = (slice(None), s, slice(None), pl.ds(first_row, rows))
        copy_out(stores, out.at[s], out_hbm.at[there], out_sems.at[s])
    wait_all(stores)


def inverse_y(r_ref, even, mixing, out_hbm, out, out_sems):
    bands, _, rows, slab = r_ref.shape
    small = rows // 4
    quarter = out.shape[-1] // 4
    pieces = slab // math.gcd(slab, 128)
    step = slab // pieces
    stores = []
    for part in range(2):
        for piece in range(pieces):
            here = slice(piece * step, (piece + 1) * step)
            waves = [
                halves(r_ref[:, part, index * small : (index + 1) * small, here].reshape(bands * small, step))
                for index in range(4)
            ]
            alternate, total = product(waves[0], even[1], TN), product(waves[3], even[0], TN)
            straight, crossed = mix(waves[1], waves[2], mixing, TN)
            plus, minus = total + alternate, total - alternate
            for q, result in enumerate((plus + straight, minus + crossed, plus - straight, minus - crossed)):
                out[part, here, q * quarter : (q + 1) * quarter] = result
            there = pl.ds(piece * step, step)
            copy_out(stores, out.at[part, there], out_hbm.at[part, there], out_sems.at[part * pieces + piece])
    wait_all(stores)


def call(kernel, operands, outs, flops, spaces, out_spaces, scratch=(), limit=20, aliases=None):
    shapes = [space(shape, jnp.int32 if space == pltpu.SMEM else f32) for shape, space in zip(outs, out_spaces)]
    traffic = sum(math.prod(x.shape) * x.dtype.itemsize for x in operands)
    traffic += sum(4 * math.prod(shape) for shape in outs)
    many = len(outs) > 1
    specs = [pl.BlockSpec(memory_space=space) for space in out_spaces]
    operands = [pltpu.with_memory_space_constraint(x, s) if s == pltpu.HBM else x for x, s in zip(operands, spaces)]
    return pl.pallas_call(
        kernel,
        in_specs=[pl.BlockSpec(memory_space=space) for space in spaces],
        out_specs=specs if many else specs[0],
        out_shape=shapes if many else shapes[0],
        scratch_shapes=list(scratch),
        input_output_aliases=aliases or {},
        cost_estimate=pl.CostEstimate(flops=flops, bytes_accessed=traffic, transcendentals=0),
        compiler_params=pltpu.CompilerParams(vmem_limit_bytes=limit * 2**20),
    )(*operands)


def on_device(residual, counts):
    slab, length_y = residual.shape[2:]
    blocks, points, spaces = (lax.axis_size(name) for name in ("block", "point", "space"))
    length_x = slab * spaces
    group = ("point", "space")
    bands = points * spaces
    small = length_y // (4 * bands)
    quarter = length_x // 4
    table_x, table_y = cas_tables(length_x), cas_tables(length_y)
    vmem, smem, hbm, sems = pltpu.VMEM, pltpu.SMEM, pltpu.HBM, pltpu.SemaphoreType.DMA
    lanes = math.gcd(slab, 128)

    def flops_y(parts):
        return 3 * 4 * slab * parts * (length_y // 4) ** 2

    sent = []
    for chunk, kinds in enumerate(CHUNKS):
        height = 2 * (slab // lanes) * len(kinds) * small + 8 * (1 - chunk)
        sent.append(
            call(
                functools.partial(forward_y, kinds, chunk),
                [counts, residual[0], *table_y],
                [(bands, height, lanes)],
                flops_y(1 if chunk else 5),
                [smem, hbm, hbm, hbm],
                [hbm],
                scratch=[
                    vmem(residual.shape[1:], f32),
                    vmem((bands, height, lanes), f32),
                    *[vmem(table.shape, bf16) for table in table_y],
                    sems((4,)),
                    sems((2,)),
                ],
            )
        )
    turns, spectra, carry = [], [], []
    shapes = []
    for chunk, kinds in enumerate(CHUNKS):
        rows = len(kinds) * small
        shapes.append(((4, points, 2, rows, quarter), (3, 2, 4, rows, quarter)))
        spectra_shape, turns_shape = shapes[-1]
        flops_x = 3 * 4 * rows * points * 6 * quarter * quarter
        turns.append(
            call(
                functools.partial(rotations, kinds, length_x, length_y),
                [],
                [turns_shape],
                40 * 4 * rows * length_x,
                [],
                [hbm],
                scratch=[vmem(turns_shape, f32), sems((3,))],
            )
        )
        folded = [vmem((4, points * 2 * rows, quarter), bf16)] * 2
        arrived = lax.all_to_all(sent[chunk], group, split_axis=0, concat_axis=0, tiled=True)
        arrived = arrived.reshape(points, spaces, arrived.shape[1], lanes)
        results = call(
            functools.partial(forward_x, chunk),
            ([near] if chunk else []) + [arrived, turns[chunk], *table_x],
            [spectra_shape, (2, rows, length_x)] + ([] if chunk else [(points,)]),
            flops_x,
            [smem] * chunk + [vmem, hbm, vmem, vmem],
            [hbm, vmem] + ([] if chunk else [smem]),
            scratch=[vmem(turns_shape, f32), *folded, vmem(spectra_shape, f32), sems((1,)), sems((4,))],
        )
        spectra.append(results[0])
        last = results[1]
        if not chunk:
            near = results[2]
        carry.append(lax.ppermute(last, "block", [(b, b + 1) for b in range(blocks - 1)]))
        if blocks > 2:
            whole = jnp.sum(near).astype(f32) * (phase_rate / (2.0 * math.pi))
            span = lax.ppermute(whole, "block", [(b, b + 1) for b in range(blocks - 1)])
            start = own_band() * small
            modulus = [modulus_at(kind, start, 0, (small, length_x), length_x, length_y) for kind in kinds]
            modulus = jnp.concatenate(modulus, axis=0)
            reach = 1
            while reach < blocks - 1:
                steps = [(b, b + reach) for b in range(blocks - reach)]
                further = lax.ppermute(carry[chunk], "block", steps)
                cosine, sine = turn(span * modulus)
                carry[chunk] = carry[chunk] + jnp.stack(
                    [
                        cosine * further[0] + sine * further[1],
                        cosine * further[1] - sine * further[0],
                    ]
                )
                span = span + lax.ppermute(span, "block", steps)
                reach *= 2
    back = None
    for chunk, kinds in enumerate(CHUNKS):
        rows = len(kinds) * small
        spectra_shape, turns_shape = shapes[chunk]
        back = call(
            functools.partial(finish_x, 1.0 / (length_x * length_y), 0 if not chunk else 4 * small - rows),
            [near, spectra[chunk], carry[chunk], turns[chunk], *table_x] + [back] * chunk,
            [(points, spaces, 2, 4 * small, slab)],
            3 * 4 * rows * points * 6 * quarter * quarter,
            [smem] + [vmem] * 5 + [hbm] * chunk,
            [hbm],
            aliases={6: 0} if chunk else None,
            scratch=[
                vmem((spaces, points, 2, rows, slab), f32),
                vmem(spectra_shape, f32),
                sems((spaces,)),
            ],
        )
    back = back.reshape(bands, 2, 4 * small, slab)
    solved = lax.all_to_all(back, group, split_axis=0, concat_axis=0, tiled=True)
    fields = call(
        inverse_y,
        [solved, *table_y],
        [(2, slab, length_y)],
        flops_y(6),
        [vmem, vmem, vmem],
        [hbm],
        scratch=[vmem((2, slab, length_y), f32), sems((2 * slab // lanes,))],
    )
    return fields[None]


CHUNKS = ((1, 2, 3), (0,))


def solution(mesh):
    times, spaces = mesh.shape["tm"], mesh.shape["space"]
    points = 4 if times % 4 == 0 else 1
    inner = Mesh(mesh.devices.reshape(times // points, points, spaces), ("block", "point", "space"))
    when = ("block", "point")
    return jax.shard_map(
        on_device,
        mesh=inner,
        in_specs=(P(when, None, "space", None), P(when)),
        out_specs=P(when, None, "space", None),
        check_vma=False,
    )
```

```python
import functools
import math

import jax
import jax.numpy as jnp
import numpy as np
from jax import lax
from jax.experimental import pallas as pl
from jax.experimental.pallas import tpu as pltpu
from jax.sharding import Mesh
from jax.sharding import PartitionSpec as P


phase_rate = 0.004
f32 = jnp.float32
bf16 = jnp.bfloat16
NN = (((1,), (0,)), ((), ()))
NT = (((1,), (1,)), ((), ()))
TN = (((0,), (0,)), ((), ()))
SIN = (3.14159274, -5.1677103, 2.55007744, -0.598291218, 0.0776574388)
COS = (1.0, -4.93480206, 4.05870914, -1.335212, 0.23493728, -0.0243962663)


def cas_tables(length):
    steps = np.arange(length // 4, dtype=np.int64)

    def cas(k):
        angle = 2.0 * np.pi * ((k[:, None] * steps[None, :]) % length) / length
        return np.cos(angle) + np.sin(angle)

    tables = []
    for pair in ((4 * steps, 4 * steps + 2), (4 * steps + 1, -4 * steps - 1)):
        table = np.stack([cas(k) for k in pair]).astype(np.float32)
        high = table.astype(jnp.bfloat16)
        low = (table - high.astype(np.float32)).astype(jnp.bfloat16)
        tables.append(np.stack([high, low], axis=1))
    return tables


def halves(value):
    high = value.astype(bf16)
    return high, (value - high.astype(f32)).astype(bf16)


def product(left, right, form):
    dot = functools.partial(lax.dot_general, dimension_numbers=form, preferred_element_type=f32)
    return dot(left[0], right[0]) + dot(left[0], right[1]) + dot(left[1], right[0])


def fold(parts):
    even, cross = parts[0] + parts[2], parts[1] + parts[3]
    return even + cross, even - cross


def mix(first, second, table, form):
    plain, turned = table[0], table[1]
    return (
        product(first, plain, form) + product(second, turned, form),
        product(first, turned, form) - product(second, plain, form),
    )


def signed_wave(indices, length):
    return jnp.where(indices < length // 2, indices, indices - length).astype(f32)


def wave_at(spot, length):
    quarter = length // 4
    block = spot // quarter
    wave = 4 * (spot % quarter) + jnp.where(block == 1, 2, jnp.where(block == 0, 0, 1))
    return jnp.where(block == 3, length - wave, wave)


def modulus_at(start, start_x, shape, length_x, length_y):
    place_y = start + lax.broadcasted_iota(jnp.int32, shape, 0)
    place_x = start_x + lax.broadcasted_iota(jnp.int32, shape, 1)
    wave_y = signed_wave(wave_at(place_y, length_y), length_y)
    wave_x = signed_wave(wave_at(place_x, length_x), length_x)
    return jnp.sqrt(wave_x * wave_x + wave_y * wave_y)


def turn(angle):
    part = angle - jnp.round(angle)
    square = part * part
    sine = jnp.full_like(square, SIN[-1])
    for factor in SIN[-2::-1]:
        sine = sine * square + factor
    sine = sine * part
    cosine = jnp.full_like(square, COS[-1])
    for factor in COS[-2::-1]:
        cosine = cosine * square + factor
    return 1.0 - 2.0 * sine * sine, 2.0 * sine * cosine


def place(odd, rows, length_y):
    band = lax.axis_index("point") * lax.axis_size("space") + lax.axis_index("space")
    return odd * (length_y // 2) + band * rows


def copy_in(pairs, sems):
    copies = [pltpu.make_async_copy(source, target, sems.at[i]) for i, (source, target) in enumerate(pairs)]
    for copy in copies:
        copy.start()
    return copies


def copy_out(copies, source, target, sem):
    copies.append(pltpu.make_async_copy(source, target, sem))
    copies[-1].start()


def wait_all(copies):
    for copy in copies:
        copy.wait()


def forward_y(odd, count_ref, x_hbm, table_hbm, out_hbm, x_ref, out, table_ref, sems, out_sems):
    pairs = [(x_hbm.at[0], x_ref.at[0]), (table_hbm, table_ref), (x_hbm.at[1], x_ref.at[1])]
    copies = copy_in(pairs, sems)
    bands, height, lanes = out.shape
    slab, length_y = x_ref.shape[1:]
    quarter = length_y // 4
    rows = length_y // (2 * bands)
    tall = slab // lanes * rows
    wait_all(copies[:-1])
    if not odd:
        out[:, 2 * tall :] = jnp.full((bands, height - 2 * tall, lanes), count_ref[0].astype(f32))
    table = table_ref[...]
    stores = []

    def keep(part, first, result):
        reach = result.shape[0] // rows
        for piece in range(slab // lanes):
            start = part * tall + piece * rows
            wanted = result[:, piece * lanes : (piece + 1) * lanes]
            out[first : first + reach, start : start + rows] = wanted.reshape(reach, rows, lanes)
        here = (pl.ds(first, reach), pl.ds(part * tall, height - tall if part else tall))
        copy_out(stores, out.at[here], out_hbm.at[here], out_sems.at[2 * part + first // reach])

    for part in range(2):
        if part:
            copies[-1].wait()
        pieces = [x_ref[part, :, q * quarter : (q + 1) * quarter] for q in range(4)]
        if odd:
            first, second = halves(pieces[0] - pieces[2]), halves(pieces[1] - pieces[3])
            plain, turned = table[0], table[1]
            keep(part, 0, product(plain, first, NT) + product(turned, second, NT))
            keep(part, bands // 2, product(turned, first, NT) - product(plain, second, NT))
        else:
            for half, value in enumerate(fold(pieces)):
                keep(part, half * bands // 2, product(table[half], halves(value), NT))
    wait_all(stores)


def rotations(odd, length_x, length_y, out_hbm, out, sems):
    _, _, choices, rows, quarter = out.shape
    block = math.gcd(rows, 8)
    start = place(odd, rows, length_y)
    stores = []
    for q in range(3):

        def step(index, _):
            here = pl.ds(pl.multiple_of(index * block, block), block)
            modulus = modulus_at(start + index * block, q * quarter, (block, quarter), length_x, length_y)
            for n in range(choices):
                rate = phase_rate * (n + 1) / (2.0 * math.pi)
                out[q, 0, n, here, :], out[q, 1, n, here, :] = turn(rate * modulus)
            return 0

        lax.fori_loop(0, rows // block, step, 0)
        copy_out(stores, out.at[q], out_hbm.at[q], sems.at[q])
    wait_all(stores)


def forward_x(odd, *refs):
    refs, (turns, highs, lows, spectra, turn_sem, out_sems) = refs[:-6], refs[-6:]
    if odd:
        count_ref, r_ref, turns_hbm, even, mixing, spectra_hbm, last_hbm, last, last_sems = refs
    else:
        r_ref, turns_hbm, even, mixing, spectra_hbm, last, count_ref = refs
    points, spaces, _, lanes = r_ref.shape
    _, _, rows, quarter = spectra.shape[1:]
    slab = 4 * quarter // spaces
    wide = slab // lanes
    tall = wide * rows
    count = 2 * rows
    turn_copy = pltpu.make_async_copy(turns_hbm, turns, turn_sem.at[0])
    turn_copy.start()
    if not odd:
        for n in range(points):
            count_ref[n] = jnp.max(r_ref[n, 0, 2 * tall :]).astype(jnp.int32)

    def gather(n, _):
        pieces = []
        for s in range(spaces):
            slices = [r_ref[n, s, start : start + rows] for start in range(0, 2 * tall, rows)]
            parts = [jnp.concatenate(slices[part * wide : (part + 1) * wide], axis=-1) for part in range(2)]
            pieces.append(jnp.concatenate(parts, axis=0))
        if spaces != 4:
            whole = jnp.concatenate(pieces, axis=-1)
            pieces = [whole[:, q * quarter : (q + 1) * quarter] for q in range(4)]
        here = pl.ds(pl.multiple_of(n * count, count), count)
        columns = [*fold(pieces), pieces[0] - pieces[2], pieces[1] - pieces[3]]
        for q, column in enumerate(columns):
            highs[q, here], lows[q, here] = halves(column)
        return 0

    lax.fori_loop(0, points, gather, 0)
    folded = [(highs[q], lows[q]) for q in range(4)]
    choice = [jnp.clip(count_ref[n] - 1, 0, turns.shape[2] - 1) for n in range(points)]
    stores = []

    def keep(q, result):
        spectra[q] = result.reshape(points, 2, rows, quarter)
        copy_out(stores, spectra.at[q], spectra_hbm.at[q], out_sems.at[q])

    for q, result in zip((2, 3), mix(*folded[2:], mixing, NT)):
        keep(q, result)
    for q in range(2):
        keep(q, product(folded[q], even[q], NT))
    turn_copy.wait()
    for q in (2, 3, 0, 1):
        first, second = spectra[q, 0, 0], spectra[q, 0, 1]
        for n in range(1, points):
            cosine, sine = turns[min(q, 2), 0, choice[n]], turns[min(q, 2), 1, choice[n]]
            first, second = (
                cosine * first + sine * second + spectra[q, n, 0],
                cosine * second - sine * first + spectra[q, n, 1],
            )
        here = slice(q * quarter, (q + 1) * quarter)
        last[0, :, here] = first
        last[1, :, here] = second
        if odd:
            there = (slice(None), slice(None), pl.ds(q * quarter, quarter))
            copy_out(stores, last.at[there], last_hbm.at[there], last_sems.at[q])
    wait_all(stores)


def finish_x(scaling, count_ref, spectra, carry, turns, even, mixing, out_hbm, out, states, out_sems, *scratch):
    if scratch:
        spectra_hbm, turns_hbm, (spectra, turns, sems) = spectra, turns, scratch
        wait_all(copy_in([(turns_hbm, turns), (spectra_hbm, spectra)], sems))
    spaces, points, _, rows, slab = out.shape
    quarter = spaces * slab // 4
    count = points * 2 * rows
    choice = [jnp.clip(count_ref[n] - 1, 0, turns.shape[2] - 1) for n in range(points)]
    for q in range(4):
        first, second = (carry[part, :, q * quarter : (q + 1) * quarter] for part in range(2))
        for n in range(points):
            cosine, sine = turns[min(q, 2), 0, choice[n]], turns[min(q, 2), 1, choice[n]]
            first, second = (
                cosine * first + sine * second + spectra[q, n, 0],
                cosine * second - sine * first + spectra[q, n, 1],
            )
            states[q, n, 0] = first * scaling
            states[q, n, 1] = second * scaling
    waves = [halves(states[q].reshape(count, quarter)) for q in range(4)]
    total, alternate = product(waves[0], even[0], NN), product(waves[1], even[1], NN)
    plus, minus = total + alternate, total - alternate
    straight, crossed = mix(waves[2], waves[3], mixing, NN)
    results = [plus + straight, minus + crossed, plus - straight, minus - crossed]
    if spaces != 4:
        whole = jnp.concatenate(results, axis=-1)
        results = [whole[:, s * slab : (s + 1) * slab] for s in range(spaces)]
    stores = []
    for s in range(spaces):
        out[s] = results[s].reshape(points, 2, rows, slab)
        copy_out(stores, out.at[s], out_hbm.at[:, s], out_sems.at[s])
    wait_all(stores)


def inverse_y_even(r_hbm, table, out_hbm, _, r_ref, out, in_sems, sems):
    wait_all(copy_in([(r_hbm, r_ref)], in_sems))
    bands, _, rows, slab = r_ref.shape
    half = bands // 2
    stores = []
    for part in range(2):
        total = product(halves(r_ref[:half, part].reshape(half * rows, slab)), table[0], TN)
        alternate = product(halves(r_ref[half:, part].reshape(half * rows, slab)), table[1], TN)
        out[part] = jnp.concatenate([total + alternate, total - alternate], axis=-1)
        copy_out(stores, out.at[part], out_hbm.at[part], sems.at[part])
    wait_all(stores)


def inverse_y_odd(r_ref, even_hbm, table, out_hbm, even, out, sems, out_sems):
    bands, _, rows, slab = r_ref.shape
    half = bands // 2
    quarter = even.shape[-1] // 2
    pieces = slab // math.gcd(slab, 128)
    step = slab // pieces
    spots = [(part, pl.ds(piece * step, step)) for part in range(2) for piece in range(pieces)]
    copies = copy_in([(even_hbm.at[spot], even.at[spot]) for spot in spots], sems)
    stores = []
    for part in range(2):
        for piece in range(pieces):
            here = slice(piece * step, (piece + 1) * step)
            first = halves(r_ref[:half, part, :, here].reshape(half * rows, step))
            second = halves(r_ref[half:, part, :, here].reshape(half * rows, step))
            results = mix(first, second, table, TN)
            copies[part * pieces + piece].wait()
            for q, result in enumerate(results):
                base = even[part, here, q * quarter : (q + 1) * quarter]
                out[part, here, q * quarter : (q + 1) * quarter] = base + result
                out[part, here, (q + 2) * quarter : (q + 3) * quarter] = base - result
            there = pl.ds(piece * step, step)
            copy_out(stores, out.at[part, there], out_hbm.at[part, there], out_sems.at[part * pieces + piece])
    wait_all(stores)


def call(kernel, operands, outs, flops, spaces, out_spaces, scratch=(), limit=20, aliases=None):
    shapes = [space(shape, jnp.int32 if space == pltpu.SMEM else f32) for shape, space in zip(outs, out_spaces)]
    traffic = sum(math.prod(x.shape) * x.dtype.itemsize for x in operands)
    traffic += sum(4 * math.prod(shape) for shape in outs)
    many = len(outs) > 1
    specs = [pl.BlockSpec(memory_space=space) for space in out_spaces]
    operands = [pltpu.with_memory_space_constraint(x, s) if s == pltpu.HBM else x for x, s in zip(operands, spaces)]
    return pl.pallas_call(
        kernel,
        in_specs=[pl.BlockSpec(memory_space=space) for space in spaces],
        out_specs=specs if many else specs[0],
        out_shape=shapes if many else shapes[0],
        scratch_shapes=list(scratch),
        input_output_aliases=aliases or {},
        cost_estimate=pl.CostEstimate(flops=flops, bytes_accessed=traffic, transcendentals=0),
        compiler_params=pltpu.CompilerParams(vmem_limit_bytes=limit * 2**20),
    )(*operands)


def on_device(residual, counts):
    slab, length_y = residual.shape[2:]
    blocks, points, spaces = (lax.axis_size(name) for name in ("block", "point", "space"))
    length_x = slab * spaces
    group = ("point", "space")
    bands = points * spaces
    rows = length_y // (2 * bands)
    quarter = length_x // 4
    table_x, tables_y = (cas_tables(length) for length in (length_x, length_y))
    flops_y = [3 * 4 * slab * (length_y // 2) * (length_y // wide) for wide in (4, 2)]
    flops_x = 3 * 4 * rows * points * length_x * 3 * length_x // 8
    vmem, smem, hbm, sems = pltpu.VMEM, pltpu.SMEM, pltpu.HBM, pltpu.SemaphoreType.DMA
    spectra_shape = (4, points, 2, rows, quarter)
    turns_shape = (3, 2, 4, rows, quarter)

    lanes = math.gcd(slab, 128)
    tall = slab // lanes * rows
    heights = (2 * tall + 8, 2 * tall)

    sent, turns = [], []
    for odd in range(2):
        table = tables_y[odd]
        sent.append(
            call(
                functools.partial(forward_y, odd),
                [counts, residual[0], table],
                [(bands, heights[odd], lanes)],
                flops_y[odd],
                [smem, hbm, hbm],
                [hbm],
                scratch=[
                    vmem(residual.shape[1:], f32),
                    vmem((bands, heights[odd], lanes), f32),
                    vmem(table.shape, bf16),
                    sems((3,)),
                    sems((4,)),
                ],
            )
        )
        turns.append(
            call(
                functools.partial(rotations, odd, length_x, length_y),
                [],
                [turns_shape],
                40 * 4 * rows * length_x,
                [],
                [hbm],
                scratch=[vmem(turns_shape, f32), sems((3,))],
            )
        )
    spectra, carry = [None] * 2, [None] * 2
    for odd in range(2):
        arrived = lax.all_to_all(sent[odd], group, split_axis=0, concat_axis=0, tiled=True)
        if odd:
            arrived, spectra[0], later = lax.optimization_barrier((arrived, spectra[0], turns[0]))
        arrived = arrived.reshape(points, spaces, heights[odd], lanes)
        folded = [vmem((4, points * 2 * rows, quarter), bf16)] * 2
        results = call(
            functools.partial(forward_x, odd),
            [near, arrived, turns[1], *table_x] if odd else [arrived, turns[0], *table_x],
            [spectra_shape, (2, rows, length_x)] + ([] if odd else [(points,)]),
            flops_x,
            [smem] * odd + [vmem, hbm, vmem, vmem],
            [hbm, hbm] if odd else [hbm, vmem, smem],
            scratch=[vmem((2, rows, length_x), f32), sems((4,))] * odd
            + [vmem(turns_shape, f32), *folded, vmem(spectra_shape, f32), sems((1,)), sems((4,))],
        )
        spectra[odd], last = results[:2]
        if not odd:
            near = results[2]
        carry[odd] = lax.ppermute(last, "block", [(b, b + 1) for b in range(blocks - 1)])
        if blocks > 2:
            total = jnp.sum(near).astype(f32) * (phase_rate / (2.0 * math.pi))
            span = lax.ppermute(total, "block", [(b, b + 1) for b in range(blocks - 1)])
            modulus = modulus_at(place(odd, rows, length_y), 0, (rows, length_x), length_x, length_y)
            reach = 1
            while reach < blocks - 1:
                steps = [(b, b + reach) for b in range(blocks - reach)]
                further = lax.ppermute(carry[odd], "block", steps)
                cosine, sine = turn(span * modulus)
                carry[odd] = carry[odd] + jnp.stack(
                    [
                        cosine * further[0] + sine * further[1],
                        cosine * further[1] - sine * further[0],
                    ]
                )
                span = span + lax.ppermute(span, "block", steps)
                reach *= 2
    carry[0], spectra[1] = lax.optimization_barrier((carry[0], spectra[1]))
    solved = []
    for odd in range(2):
        back = call(
            functools.partial(finish_x, 1.0 / (length_x * length_y)),
            [near, spectra[odd], carry[odd], turns[1] if odd else later, *table_x],
            [(points, spaces, 2, rows, slab)],
            flops_x,
            [smem, hbm, vmem, hbm, vmem, vmem] if odd else [smem] + [vmem] * 5,
            [hbm],
            scratch=[
                vmem((spaces, points, 2, rows, slab), f32),
                vmem(spectra_shape, f32),
                sems((spaces,)),
            ]
            + [vmem(spectra_shape, f32), vmem(turns_shape, f32), sems((2,))] * odd,
        )
        back = back.reshape(bands, 2, rows, slab)
        solved.append(lax.all_to_all(back, group, split_axis=0, concat_axis=0, tiled=True))
    half = (2, slab, length_y // 2)
    even, _ = call(
        inverse_y_even,
        [solved[0], tables_y[0]],
        [half, solved[0].shape],
        flops_y[0],
        [hbm, vmem],
        [hbm, hbm],
        aliases={0: 1},
        scratch=[vmem((bands, 2, rows, slab), f32), vmem(half, f32), sems((1,)), sems((2,))],
    )
    fields = call(
        inverse_y_odd,
        [solved[1], even, tables_y[1]],
        [(2, slab, length_y)],
        flops_y[1],
        [vmem, hbm, vmem],
        [hbm],
        scratch=[vmem(half, f32), vmem((2, slab, length_y), f32), sems((2 * slab // lanes,)), sems((2 * slab // lanes,))],
    )
    return fields[None]


def solution(mesh):
    times, spaces = mesh.shape["tm"], mesh.shape["space"]
    points = 4 if times % 4 == 0 else 1
    inner = Mesh(mesh.devices.reshape(times // points, points, spaces), ("block", "point", "space"))
    when = ("block", "point")
    return jax.shard_map(
        on_device,
        mesh=inner,
        in_specs=(P(when, None, "space", None), P(when)),
        out_specs=P(when, None, "space", None),
        check_vma=False,
    )
```

```python
import functools
import math

import jax
import jax.numpy as jnp
import numpy as np
from jax import lax
from jax.experimental import pallas as pl
from jax.experimental.pallas import tpu as pltpu
from jax.sharding import Mesh
from jax.sharding import PartitionSpec as P


phase_rate = 0.004
f32 = jnp.float32
bf16 = jnp.bfloat16
NN = (((1,), (0,)), ((), ()))
NT = (((1,), (1,)), ((), ()))
TN = (((0,), (0,)), ((), ()))
SIN = (3.14159274, -5.1677103, 2.55007744, -0.598291218, 0.0776574388)
COS = (1.0, -4.93480206, 4.05870914, -1.335212, 0.23493728, -0.0243962663)


def cas_tables(length):
    steps = np.arange(length // 4, dtype=np.int64)

    def cas(k):
        angle = 2.0 * np.pi * ((k[:, None] * steps[None, :]) % length) / length
        return np.cos(angle) + np.sin(angle)

    tables = []
    for pair in ((4 * steps, 4 * steps + 2), (4 * steps + 1, -4 * steps - 1)):
        table = np.stack([cas(k) for k in pair]).astype(np.float32)
        high = table.astype(jnp.bfloat16)
        low = (table - high.astype(np.float32)).astype(jnp.bfloat16)
        tables.append(np.stack([high, low], axis=1))
    return tables


def halves(value):
    high = value.astype(bf16)
    return high, (value - high.astype(f32)).astype(bf16)


def product(left, right, form):
    dot = functools.partial(lax.dot_general, dimension_numbers=form, preferred_element_type=f32)
    return dot(left[0], right[0]) + dot(left[0], right[1]) + dot(left[1], right[0])


def fold(parts):
    even, cross = parts[0] + parts[2], parts[1] + parts[3]
    return even + cross, even - cross


def mix(first, second, table, form):
    plain, turned = table[0], table[1]
    return (
        product(first, plain, form) + product(second, turned, form),
        product(first, turned, form) - product(second, plain, form),
    )


def signed_wave(indices, length):
    return jnp.where(indices < length // 2, indices, indices - length).astype(f32)


def wave_at(spot, length):
    quarter = length // 4
    block = spot // quarter
    wave = 4 * (spot % quarter) + jnp.where(block == 1, 2, jnp.where(block == 0, 0, 1))
    return jnp.where(block == 3, length - wave, wave)


def modulus_at(start, start_x, shape, length_x, length_y):
    place_y = start + lax.broadcasted_iota(jnp.int32, shape, 0)
    place_x = start_x + lax.broadcasted_iota(jnp.int32, shape, 1)
    wave_y = signed_wave(wave_at(place_y, length_y), length_y)
    wave_x = signed_wave(wave_at(place_x, length_x), length_x)
    return jnp.sqrt(wave_x * wave_x + wave_y * wave_y)


def turn(angle):
    part = angle - jnp.round(angle)
    square = part * part
    sine = jnp.full_like(square, SIN[-1])
    for factor in SIN[-2::-1]:
        sine = sine * square + factor
    sine = sine * part
    cosine = jnp.full_like(square, COS[-1])
    for factor in COS[-2::-1]:
        cosine = cosine * square + factor
    return 1.0 - 2.0 * sine * sine, 2.0 * sine * cosine


def place(odd, rows, length_y):
    band = lax.axis_index("point") * lax.axis_size("space") + lax.axis_index("space")
    return odd * (length_y // 2) + band * rows


def copy_in(pairs, sems):
    copies = [pltpu.make_async_copy(source, target, sems.at[i]) for i, (source, target) in enumerate(pairs)]
    for copy in copies:
        copy.start()
    return copies


def copy_out(copies, source, target, sem):
    copies.append(pltpu.make_async_copy(source, target, sem))
    copies[-1].start()


def wait_all(copies):
    for copy in copies:
        copy.wait()


def forward_y(odd, count_ref, x_hbm, table_hbm, out_hbm, x_ref, out, table_ref, sems, out_sems):
    pairs = [(x_hbm.at[0], x_ref.at[0]), (table_hbm, table_ref), (x_hbm.at[1], x_ref.at[1])]
    copies = copy_in(pairs, sems)
    bands, height, lanes = out.shape
    slab, length_y = x_ref.shape[1:]
    quarter = length_y // 4
    rows = length_y // (2 * bands)
    tall = slab // lanes * rows
    wait_all(copies[:-1])
    if not odd:
        out[:, 2 * tall :] = jnp.full((bands, height - 2 * tall, lanes), count_ref[0].astype(f32))
    table = table_ref[...]
    stores = []

    def keep(part, first, result):
        reach = result.shape[0] // rows
        for piece in range(slab // lanes):
            start = part * tall + piece * rows
            wanted = result[:, piece * lanes : (piece + 1) * lanes]
            out[first : first + reach, start : start + rows] = wanted.reshape(reach, rows, lanes)

    for part in range(2):
        if part:
            copies[-1].wait()
        pieces = [x_ref[part, :, q * quarter : (q + 1) * quarter] for q in range(4)]
        if odd:
            first, second = halves(pieces[0] - pieces[2]), halves(pieces[1] - pieces[3])
            plain, turned = table[0], table[1]
            keep(part, 0, product(plain, first, NT) + product(turned, second, NT))
            keep(part, bands // 2, product(turned, first, NT) - product(plain, second, NT))
        else:
            for half, value in enumerate(fold(pieces)):
                keep(part, half * bands // 2, product(table[half], halves(value), NT))
        here = pl.ds(part * tall, height - tall if part else tall)
        copy_out(stores, out.at[:, here], out_hbm.at[:, here], out_sems.at[part])
    wait_all(stores)


def rotations(odd, length_x, length_y, out_hbm, out, sems):
    _, _, choices, rows, quarter = out.shape
    block = math.gcd(rows, 8)
    start = place(odd, rows, length_y)
    stores = []
    for q in range(3):

        def step(index, _):
            here = pl.ds(pl.multiple_of(index * block, block), block)
            modulus = modulus_at(start + index * block, q * quarter, (block, quarter), length_x, length_y)
            for n in range(choices):
                rate = phase_rate * (n + 1) / (2.0 * math.pi)
                out[q, 0, n, here, :], out[q, 1, n, here, :] = turn(rate * modulus)
            return 0

        lax.fori_loop(0, rows // block, step, 0)
        copy_out(stores, out.at[q], out_hbm.at[q], sems.at[q])
    wait_all(stores)


def forward_x(odd, *refs):
    refs, (turns, highs, lows, spectra, turn_sem, out_sems) = refs[:-6], refs[-6:]
    if odd:
        count_ref, r_ref, turns_hbm, even, mixing, spectra_hbm, last_hbm, last, last_sems = refs
    else:
        r_ref, turns_hbm, even, mixing, spectra_hbm, last, count_ref = refs
    points, spaces, _, lanes = r_ref.shape
    _, _, rows, quarter = spectra.shape[1:]
    slab = 4 * quarter // spaces
    wide = slab // lanes
    tall = wide * rows
    count = 2 * rows
    turn_copy = pltpu.make_async_copy(turns_hbm, turns, turn_sem.at[0])
    turn_copy.start()
    if not odd:
        for n in range(points):
            count_ref[n] = jnp.max(r_ref[n, 0, 2 * tall :]).astype(jnp.int32)

    def gather(n, _):
        pieces = []
        for s in range(spaces):
            slices = [r_ref[n, s, start : start + rows] for start in range(0, 2 * tall, rows)]
            parts = [jnp.concatenate(slices[part * wide : (part + 1) * wide], axis=-1) for part in range(2)]
            pieces.append(jnp.concatenate(parts, axis=0))
        if spaces != 4:
            whole = jnp.concatenate(pieces, axis=-1)
            pieces = [whole[:, q * quarter : (q + 1) * quarter] for q in range(4)]
        here = pl.ds(pl.multiple_of(n * count, count), count)
        columns = [*fold(pieces), pieces[0] - pieces[2], pieces[1] - pieces[3]]
        for q, column in enumerate(columns):
            highs[q, here], lows[q, here] = halves(column)
        return 0

    lax.fori_loop(0, points, gather, 0)
    folded = [(highs[q], lows[q]) for q in range(4)]
    choice = [jnp.clip(count_ref[n] - 1, 0, turns.shape[2] - 1) for n in range(points)]
    stores = []

    def keep(q, result):
        spectra[q] = result.reshape(points, 2, rows, quarter)
        copy_out(stores, spectra.at[q], spectra_hbm.at[q], out_sems.at[q])

    for q, result in zip((2, 3), mix(*folded[2:], mixing, NT)):
        keep(q, result)
    for q in range(2):
        keep(q, product(folded[q], even[q], NT))
    turn_copy.wait()
    for q in (2, 3, 0, 1):
        first, second = spectra[q, 0, 0], spectra[q, 0, 1]
        for n in range(1, points):
            cosine, sine = turns[min(q, 2), 0, choice[n]], turns[min(q, 2), 1, choice[n]]
            first, second = (
                cosine * first + sine * second + spectra[q, n, 0],
                cosine * second - sine * first + spectra[q, n, 1],
            )
        here = slice(q * quarter, (q + 1) * quarter)
        last[0, :, here] = first
        last[1, :, here] = second
        if odd:
            there = (slice(None), slice(None), pl.ds(q * quarter, quarter))
            copy_out(stores, last.at[there], last_hbm.at[there], last_sems.at[q])
    wait_all(stores)


def finish_x(scaling, count_ref, spectra, carry, turns, even, mixing, out_hbm, out, states, out_sems, *scratch):
    if scratch:
        spectra_hbm, turns_hbm, (spectra, turns, sems) = spectra, turns, scratch
        wait_all(copy_in([(turns_hbm, turns), (spectra_hbm, spectra)], sems))
    spaces, points, _, rows, slab = out.shape
    quarter = spaces * slab // 4
    count = points * 2 * rows
    choice = [jnp.clip(count_ref[n] - 1, 0, turns.shape[2] - 1) for n in range(points)]
    for q in range(4):
        first, second = (carry[part, :, q * quarter : (q + 1) * quarter] for part in range(2))
        for n in range(points):
            cosine, sine = turns[min(q, 2), 0, choice[n]], turns[min(q, 2), 1, choice[n]]
            first, second = (
                cosine * first + sine * second + spectra[q, n, 0],
                cosine * second - sine * first + spectra[q, n, 1],
            )
            states[q, n, 0] = first * scaling
            states[q, n, 1] = second * scaling
    waves = [halves(states[q].reshape(count, quarter)) for q in range(4)]
    total, alternate = product(waves[0], even[0], NN), product(waves[1], even[1], NN)
    plus, minus = total + alternate, total - alternate
    straight, crossed = mix(waves[2], waves[3], mixing, NN)
    results = [plus + straight, minus + crossed, plus - straight, minus - crossed]
    if spaces != 4:
        whole = jnp.concatenate(results, axis=-1)
        results = [whole[:, s * slab : (s + 1) * slab] for s in range(spaces)]
    stores = []
    for s in range(spaces):
        out[s] = results[s].reshape(points, 2, rows, slab)
        copy_out(stores, out.at[s], out_hbm.at[:, s], out_sems.at[s])
    wait_all(stores)


def inverse_y_even(r_hbm, table, out_hbm, _, r_ref, out, in_sems, sems):
    wait_all(copy_in([(r_hbm, r_ref)], in_sems))
    bands, _, rows, slab = r_ref.shape
    half = bands // 2
    stores = []
    for part in range(2):
        total = product(halves(r_ref[:half, part].reshape(half * rows, slab)), table[0], TN)
        alternate = product(halves(r_ref[half:, part].reshape(half * rows, slab)), table[1], TN)
        out[part] = jnp.concatenate([total + alternate, total - alternate], axis=-1)
        copy_out(stores, out.at[part], out_hbm.at[part], sems.at[part])
    wait_all(stores)


def inverse_y_odd(r_ref, even_hbm, table, out_hbm, even, out, sems, out_sems):
    bands, _, rows, slab = r_ref.shape
    half = bands // 2
    quarter = even.shape[-1] // 2
    pieces = slab // math.gcd(slab, 128)
    step = slab // pieces
    copies = copy_in([(even_hbm, even)], sems)
    stores = []
    for part in range(2):
        for piece in range(pieces):
            here = slice(piece * step, (piece + 1) * step)
            first = halves(r_ref[:half, part, :, here].reshape(half * rows, step))
            second = halves(r_ref[half:, part, :, here].reshape(half * rows, step))
            results = mix(first, second, table, TN)
            if not stores:
                wait_all(copies)
            for q, result in enumerate(results):
                base = even[part, here, q * quarter : (q + 1) * quarter]
                out[part, here, q * quarter : (q + 1) * quarter] = base + result
                out[part, here, (q + 2) * quarter : (q + 3) * quarter] = base - result
            there = pl.ds(piece * step, step)
            copy_out(stores, out.at[part, there], out_hbm.at[part, there], out_sems.at[part * pieces + piece])
    wait_all(stores)


def call(kernel, operands, outs, flops, spaces, out_spaces, scratch=(), limit=20, aliases=None):
    shapes = [space(shape, jnp.int32 if space == pltpu.SMEM else f32) for shape, space in zip(outs, out_spaces)]
    traffic = sum(math.prod(x.shape) * x.dtype.itemsize for x in operands)
    traffic += sum(4 * math.prod(shape) for shape in outs)
    many = len(outs) > 1
    specs = [pl.BlockSpec(memory_space=space) for space in out_spaces]
    operands = [pltpu.with_memory_space_constraint(x, s) if s == pltpu.HBM else x for x, s in zip(operands, spaces)]
    return pl.pallas_call(
        kernel,
        in_specs=[pl.BlockSpec(memory_space=space) for space in spaces],
        out_specs=specs if many else specs[0],
        out_shape=shapes if many else shapes[0],
        scratch_shapes=list(scratch),
        input_output_aliases=aliases or {},
        cost_estimate=pl.CostEstimate(flops=flops, bytes_accessed=traffic, transcendentals=0),
        compiler_params=pltpu.CompilerParams(vmem_limit_bytes=limit * 2**20),
    )(*operands)


def on_device(residual, counts):
    slab, length_y = residual.shape[2:]
    blocks, points, spaces = (lax.axis_size(name) for name in ("block", "point", "space"))
    length_x = slab * spaces
    group = ("point", "space")
    bands = points * spaces
    rows = length_y // (2 * bands)
    quarter = length_x // 4
    table_x, tables_y = (cas_tables(length) for length in (length_x, length_y))
    flops_y = [3 * 4 * slab * (length_y // 2) * (length_y // wide) for wide in (4, 2)]
    flops_x = 3 * 4 * rows * points * length_x * 3 * length_x // 8
    vmem, smem, hbm, sems = pltpu.VMEM, pltpu.SMEM, pltpu.HBM, pltpu.SemaphoreType.DMA
    spectra_shape = (4, points, 2, rows, quarter)
    turns_shape = (3, 2, 4, rows, quarter)

    lanes = math.gcd(slab, 128)
    tall = slab // lanes * rows
    heights = (2 * tall + 8, 2 * tall)

    sent, turns = [], []
    for odd in range(2):
        table = tables_y[odd]
        sent.append(
            call(
                functools.partial(forward_y, odd),
                [counts, residual[0], table],
                [(bands, heights[odd], lanes)],
                flops_y[odd],
                [smem, hbm, hbm],
                [hbm],
                scratch=[
                    vmem(residual.shape[1:], f32),
                    vmem((bands, heights[odd], lanes), f32),
                    vmem(table.shape, bf16),
                    sems((3,)),
                    sems((2,)),
                ],
            )
        )
        turns.append(
            call(
                functools.partial(rotations, odd, length_x, length_y),
                [],
                [turns_shape],
                40 * 4 * rows * length_x,
                [],
                [hbm],
                scratch=[vmem(turns_shape, f32), sems((3,))],
            )
        )
    spectra, carry = [None] * 2, [None] * 2
    for odd in range(2):
        arrived = lax.all_to_all(sent[odd], group, split_axis=0, concat_axis=0, tiled=True)
        if odd:
            arrived, spectra[0], later = lax.optimization_barrier((arrived, spectra[0], turns[0]))
        arrived = arrived.reshape(points, spaces, heights[odd], lanes)
        folded = [vmem((4, points * 2 * rows, quarter), bf16)] * 2
        results = call(
            functools.partial(forward_x, odd),
            [near, arrived, turns[1], *table_x] if odd else [arrived, turns[0], *table_x],
            [spectra_shape, (2, rows, length_x)] + ([] if odd else [(points,)]),
            flops_x,
            [smem] * odd + [vmem, hbm, vmem, vmem],
            [hbm, hbm] if odd else [hbm, vmem, smem],
            scratch=[vmem((2, rows, length_x), f32), sems((4,))] * odd
            + [vmem(turns_shape, f32), *folded, vmem(spectra_shape, f32), sems((1,)), sems((4,))],
        )
        spectra[odd], last = results[:2]
        if not odd:
            near = results[2]
        carry[odd] = lax.ppermute(last, "block", [(b, b + 1) for b in range(blocks - 1)])
        if blocks > 2:
            total = jnp.sum(near).astype(f32) * (phase_rate / (2.0 * math.pi))
            span = lax.ppermute(total, "block", [(b, b + 1) for b in range(blocks - 1)])
            modulus = modulus_at(place(odd, rows, length_y), 0, (rows, length_x), length_x, length_y)
            reach = 1
            while reach < blocks - 1:
                steps = [(b, b + reach) for b in range(blocks - reach)]
                further = lax.ppermute(carry[odd], "block", steps)
                cosine, sine = turn(span * modulus)
                carry[odd] = carry[odd] + jnp.stack(
                    [
                        cosine * further[0] + sine * further[1],
                        cosine * further[1] - sine * further[0],
                    ]
                )
                span = span + lax.ppermute(span, "block", steps)
                reach *= 2
    solved = []
    for odd in range(2):
        back = call(
            functools.partial(finish_x, 1.0 / (length_x * length_y)),
            [near, spectra[odd], carry[odd], turns[1] if odd else later, *table_x],
            [(points, spaces, 2, rows, slab)],
            flops_x,
            [smem, hbm, vmem, hbm, vmem, vmem] if odd else [smem] + [vmem] * 5,
            [hbm],
            scratch=[
                vmem((spaces, points, 2, rows, slab), f32),
                vmem(spectra_shape, f32),
                sems((spaces,)),
            ]
            + [vmem(spectra_shape, f32), vmem(turns_shape, f32), sems((2,))] * odd,
        )
        back = back.reshape(bands, 2, rows, slab)
        solved.append(lax.all_to_all(back, group, split_axis=0, concat_axis=0, tiled=True))
    half = (2, slab, length_y // 2)
    even, _ = call(
        inverse_y_even,
        [solved[0], tables_y[0]],
        [half, solved[0].shape],
        flops_y[0],
        [hbm, vmem],
        [hbm, hbm],
        aliases={0: 1},
        scratch=[vmem((bands, 2, rows, slab), f32), vmem(half, f32), sems((1,)), sems((2,))],
    )
    fields = call(
        inverse_y_odd,
        [solved[1], even, tables_y[1]],
        [(2, slab, length_y)],
        flops_y[1],
        [vmem, hbm, vmem],
        [hbm],
        scratch=[vmem(half, f32), vmem((2, slab, length_y), f32), sems((1,)), sems((2 * slab // lanes,))],
    )
    return fields[None]


def solution(mesh):
    times, spaces = mesh.shape["tm"], mesh.shape["space"]
    points = 4 if times % 4 == 0 else 1
    inner = Mesh(mesh.devices.reshape(times // points, points, spaces), ("block", "point", "space"))
    when = ("block", "point")
    return jax.shard_map(
        on_device,
        mesh=inner,
        in_specs=(P(when, None, "space", None), P(when)),
        out_specs=P(when, None, "space", None),
        check_vma=False,
    )
```
